128 devices in a mesh: dp: 1, cp: 128 (over z, y, x, core).
Axes of the slice: x: 4, y: 4, z: 4, core: 2. Of those that a mesh axis runs over, the one named last changes fastest.
Arguments:
- hidden: bfloat16 [65536, 3072], P(('dp', 'cp'))
- w_q: bfloat16 [3072, 24, 128], replicated
- w_k: bfloat16 [3072, 2, 128], replicated
- w_v: bfloat16 [3072, 2, 128], replicated
- w_o: bfloat16 [24, 128, 3072], replicated
Outputs:
- output: bfloat16 [65536, 3072], P(('dp', 'cp'))
All inputs are finite; a program needn't handle non-finite values.
Results may differ from the reference program's by a relative error of at most 0.00541686.
Values are sent between devices in bfloat16 or wider.
A program may use at most 1 GiB of HBM per device.

```python
import jax
import jax.numpy as jnp
from jax import lax

CP_SIZE = 128
CHUNK = 256
MODEL_DIM = 3072
HEADS = 24
KV_HEADS = 2
HEAD_DIM = 128
WINDOW = 4096
ROPE_BASE = 10000


def setup_inputs(seed: int = 0, part: int = 0) -> dict:
    seq_len = 2 * CP_SIZE * CHUNK
    weight_keys = jax.random.split(jax.random.key(seed), 4)
    part_key = jax.random.fold_in(jax.random.key(seed + 1), part)
    noise_key, chunk_key = jax.random.split(part_key)
    token_noise = jax.random.normal(noise_key, (2 * CP_SIZE, CHUNK, MODEL_DIM), jnp.float32)
    chunk_means = jax.random.normal(chunk_key, (2 * CP_SIZE, 1, MODEL_DIM), jnp.float32)
    natural = 0.6 * token_noise + 0.8 * chunk_means
    stored = jnp.stack([natural[:CP_SIZE], natural[CP_SIZE:][::-1]], axis=1).reshape(seq_len, MODEL_DIM)
    in_scale = MODEL_DIM ** -0.5
    out_scale = (HEADS * HEAD_DIM) ** -0.5
    w_q = jax.random.normal(weight_keys[0], (MODEL_DIM, HEADS, HEAD_DIM), jnp.float32) * in_scale
    w_k = jax.random.normal(weight_keys[1], (MODEL_DIM, KV_HEADS, HEAD_DIM), jnp.float32) * in_scale
    w_v = jax.random.normal(weight_keys[2], (MODEL_DIM, KV_HEADS, HEAD_DIM), jnp.float32) * in_scale
    w_o = jax.random.normal(weight_keys[3], (HEADS, HEAD_DIM, MODEL_DIM), jnp.float32) * out_scale
    return {'hidden': stored.astype(jnp.bfloat16), 'w_q': w_q.astype(jnp.bfloat16), 'w_k': w_k.astype(jnp.bfloat16), 'w_v': w_v.astype(jnp.bfloat16), 'w_o': w_o.astype(jnp.bfloat16)}


def rotate(values, positions, factor):
    half_dim = values.shape[-1] // 2
    inv_freq = 1.0 / (ROPE_BASE ** (jnp.arange(half_dim, dtype=jnp.float32) * (2.0 / values.shape[-1])))
    angles = positions.astype(jnp.float32)[..., None, None] * inv_freq
    cos_part = jnp.cos(angles)
    sin_part = jnp.sin(angles)
    first_half = values[..., :half_dim].astype(jnp.float32)
    second_half = values[..., half_dim:].astype(jnp.float32)
    rotated = jnp.concatenate([first_half * cos_part - second_half * sin_part, second_half * cos_part + first_half * sin_part], axis=-1)
    return (rotated * factor).astype(jnp.bfloat16)


def to_natural(stored):
    blocks = stored.reshape((CP_SIZE, 2, CHUNK) + stored.shape[1:])
    return jnp.concatenate([blocks[:, 0], blocks[::-1, 1]], axis=0).reshape(stored.shape)


def to_stored(natural):
    blocks = natural.reshape((2 * CP_SIZE, CHUNK) + natural.shape[1:])
    return jnp.stack([blocks[:CP_SIZE], blocks[CP_SIZE:][::-1]], axis=1).reshape(natural.shape)


def reference(hidden, w_q, w_k, w_v, w_o):
    seq_len = hidden.shape[0]
    group_size = HEADS // KV_HEADS
    dev_ids = jnp.arange(CP_SIZE)[:, None]
    chunk_ids = jnp.concatenate([dev_ids, 2 * CP_SIZE - 1 - dev_ids], axis=1)
    positions = (chunk_ids[:, :, None] * CHUNK + jnp.arange(CHUNK)).reshape(seq_len)
    q_flat = jnp.dot(hidden, w_q.reshape(MODEL_DIM, HEADS * HEAD_DIM), preferred_element_type=jnp.float32).astype(jnp.bfloat16)
    k_flat = jnp.dot(hidden, w_k.reshape(MODEL_DIM, KV_HEADS * HEAD_DIM), preferred_element_type=jnp.float32).astype(jnp.bfloat16)
    v_flat = jnp.dot(hidden, w_v.reshape(MODEL_DIM, KV_HEADS * HEAD_DIM), preferred_element_type=jnp.float32).astype(jnp.bfloat16)
    q_nat = to_natural(rotate(q_flat.reshape(seq_len, HEADS, HEAD_DIM), positions, HEAD_DIM ** -0.5))
    k_nat = to_natural(rotate(k_flat.reshape(seq_len, KV_HEADS, HEAD_DIM), positions, 1.0))
    v_nat = to_natural(v_flat.reshape(seq_len, KV_HEADS, HEAD_DIM))
    block_rows = min(CHUNK, 128)
    key_span = WINDOW + block_rows
    pad_zeros = jnp.zeros((WINDOW, KV_HEADS, HEAD_DIM), jnp.bfloat16)
    k_pad = jnp.concatenate([pad_zeros, k_nat], axis=0)
    v_pad = jnp.concatenate([pad_zeros, v_nat], axis=0)

    def one_block(block_id):
        row_start = block_id * block_rows
        q_part = lax.dynamic_slice_in_dim(q_nat, row_start, block_rows, axis=0).reshape(block_rows, KV_HEADS, group_size, HEAD_DIM)
        k_part = lax.dynamic_slice_in_dim(k_pad, row_start, key_span, axis=0)
        v_part = lax.dynamic_slice_in_dim(v_pad, row_start, key_span, axis=0)
        q_pos = row_start + jnp.arange(block_rows)
        k_pos = row_start - WINDOW + jnp.arange(key_span)
        allowed = (k_pos[None, :] <= q_pos[:, None]) & (q_pos[:, None] - k_pos[None, :] < WINDOW) & (k_pos[None, :] >= 0)
        scores = jnp.einsum('qkgd,skd->kgqs', q_part.astype(jnp.float32), k_part.astype(jnp.float32))
        scores = jnp.where(allowed, scores, -jnp.inf)
        row_max = jnp.max(scores, axis=-1, keepdims=True)
        exp_scores = jnp.exp(scores - row_max)
        row_sum = jnp.sum(exp_scores, axis=-1)
        attn_out = jnp.einsum('kgqs,skd->qkgd', exp_scores.astype(jnp.bfloat16).astype(jnp.float32), v_part.astype(jnp.float32))
        attn_out = attn_out / jnp.transpose(row_sum, (2, 0, 1))[..., None]
        return attn_out.astype(jnp.bfloat16).reshape(block_rows, HEADS * HEAD_DIM)

    o_nat = lax.map(one_block, jnp.arange(seq_len // block_rows)).reshape(seq_len, HEADS * HEAD_DIM)
    o_stored = to_stored(o_nat)
    return jnp.dot(o_stored, w_o.reshape(HEADS * HEAD_DIM, MODEL_DIM), preferred_element_type=jnp.float32).astype(jnp.bfloat16)
```

```python
import functools

import jax
import jax.numpy as jnp
from jax import lax
from jax.experimental import pallas as pl
from jax.experimental.pallas import tpu as pltpu
from jax.sharding import PartitionSpec as P

WINDOW = 4096
ROPE_BASE = 10000.0
CHUNK = 256
REACH = WINDOW // CHUNK
GROUP = 4
STEPS = REACH // GROUP
HEADS = 24
KV_HEADS = 2
SHARE = HEADS // KV_HEADS
DIM = 128
NEG = -1e30
MESH = pl.DeviceIdType.MESH

OFFSETS = (16, 2, 1, 4, 3, 6, 5, 8, 7, 10, 9, 12, 11, 14, 13, 15)
SLOT = {offset: slot for slot, offset in enumerate(OFFSETS)}
NEAR = (8, 1, 2, 3, 4, 5, 6, 7)


def rotation(positions):
    inv_freq = 1.0 / (ROPE_BASE ** (jnp.arange(DIM // 2, dtype=jnp.float32) * (2.0 / DIM)))
    angles = positions.astype(jnp.float32)[..., None, None] * inv_freq
    return jnp.cos(angles), jnp.sin(angles)


def rotate(values, cos_part, sin_part, factor):
    first = values[..., : DIM // 2].astype(jnp.float32)
    second = values[..., DIM // 2 :].astype(jnp.float32)
    rotated = jnp.concatenate([first * cos_part - second * sin_part, second * cos_part + first * sin_part], axis=-1)
    return (rotated * factor).astype(jnp.bfloat16)


def fold8(values, op):
    return op(values.reshape(values.shape[0] // 8, 8, values.shape[1]), axis=0)


def attention_kernel(cp, q_ref, k_ref, v_ref, o_ref, kbuf, vbuf, s_a, s_b, p_a, p_b, x_a, x_b, al_a, al_b, acc, mrun, lrun, send_sem, fwd_sem, recv_sem):
    me = lax.axis_index("cp")
    chunk_of = (me, 2 * cp - 1 - me)
    even_of = (lax.rem(me, 2) == 0, lax.rem(me, 2) == 1)
    partner = me + 1 - 2 * lax.rem(me, 2)

    def direct(role, t):
        if role == 0:
            there = me + 2 * t
            low = there < cp
            return None, jnp.where(low, there, 2 * cp - 1 - there), jnp.where(low, 0, 1)
        return me >= 2 * t, me - 2 * t, 1

    def copies(src_k, src_v, band, slot, sems, device):
        for kind, (src, dst) in enumerate(((src_k, kbuf), (src_v, vbuf))):
            yield pltpu.make_async_remote_copy(
                src_ref=src, dst_ref=dst.at[band, :, slot], send_sem=sems.at[kind], recv_sem=recv_sem.at[band, slot, kind],
                device_id={"cp": device}, device_id_type=MESH)

    def when(cond, fn):
        if cond is None:
            fn()
        else:
            pl.when(cond)(fn)

    for slot, offset in enumerate(OFFSETS):
        @pl.when(me < offset)
        def _(slot=slot):
            kbuf[0, :, slot] = jnp.zeros((KV_HEADS, CHUNK, DIM), jnp.bfloat16)
            vbuf[0, :, slot] = jnp.zeros((KV_HEADS, DIM, CHUNK), jnp.bfloat16)

    barrier = pltpu.get_barrier_semaphore()
    pl.semaphore_signal(barrier, inc=1, device_id={"cp": partner}, device_id_type=MESH)
    for role in range(2):
        for t in NEAR:
            runs, device, _ = direct(role, t)
            when(runs, lambda device=device: pl.semaphore_signal(barrier, inc=1, device_id={"cp": device}, device_id_type=MESH))
    pl.semaphore_wait(barrier, 1 + len(NEAR) + jnp.minimum(len(NEAR), me // 2))

    for t in NEAR:
        for role in range(2):
            runs, device, band = direct(role, t)

            def send(role=role, t=t, device=device, band=band):
                for copy in copies(k_ref.at[role], v_ref.at[role], band, SLOT[2 * t], send_sem.at[role, t - 1], device):
                    copy.start()
            when(runs, send)

    def forward_copies(role, e):
        even = even_of[role]
        slot = jnp.where(even, SLOT[min(e + 1, REACH - 1)], SLOT[max(e - 1, 1)])
        src = (k_ref.at[role], v_ref.at[role]) if e == 0 else (kbuf.at[role, :, SLOT[e]], vbuf.at[role, :, SLOT[e]])
        return copies(*src, role, slot, fwd_sem.at[role, e // 2], partner)

    def forwards(role, e):
        even = even_of[role]
        mine = even if e == 0 else (jnp.logical_not(even) if e == REACH else None)
        if role == 0 and e > 0:
            there = me >= e
            return there if mine is None else jnp.logical_and(mine, there)
        return mine

    def wait_slot(role, slot):
        def wait():
            for copy in copies(k_ref.at[role], v_ref.at[role], role, slot, send_sem.at[role, 0], partner):
                copy.wait_recv()
        when(None if role else me >= OFFSETS[slot], wait)

    def receive_direct(role, group):
        for slot in range(GROUP * group, GROUP * group + GROUP):
            e = OFFSETS[slot]
            if e % 2 == 0:
                wait_slot(role, slot)

                def push(e=e):
                    for copy in forward_copies(role, e):
                        copy.start()
                when(forwards(role, e), push)

    def receive_forwarded(role, group):
        for slot in range(GROUP * group, GROUP * group + GROUP):
            if OFFSETS[slot] % 2:
                wait_slot(role, slot)

    for role in range(2):
        def push(role=role):
            for copy in forward_copies(role, 0):
                copy.start()
        when(forwards(role, 0), push)

    key_ids = lax.broadcasted_iota(jnp.int32, (CHUNK, CHUNK), 0)
    query_ids = lax.broadcasted_iota(jnp.int32, (CHUNK, CHUNK), 1)

    def query(role, h):
        return q_ref[pl.ds(pl.multiple_of(role * CHUNK, CHUNK), CHUNK), pl.ds(pl.multiple_of(h * DIM, DIM), DIM)]

    def scores(keys, qh):
        return lax.dot_general(keys, qh, (((1,), (1,)), ((), ())), preferred_element_type=jnp.float32)

    def bias_of(role, slot, offset):
        return jnp.where(jnp.logical_and(role == 0, me < offset), jnp.float32(NEG), jnp.float32(0))

    def offset_of(slot):
        odd = lax.rem(slot, 2)
        return jnp.where(slot == REACH - 1, REACH - 1, jnp.where(odd == 1, slot + 1, slot - 1))

    def stage_qk(role, group, h, s_ref, x_ref, first):
        kv = h // SHARE
        qh = query(role, h)
        top = None
        for c in range(GROUP):
            slot = GROUP * group + c
            s = scores(kbuf[role, kv, slot], qh)
            if first and c == 0:
                own = scores(k_ref[role, kv], qh)
                s = jnp.where(key_ids <= query_ids, own, s + bias_of(role, slot, REACH))
                part = fold8(s, jnp.max)
            else:
                offset = OFFSETS[c] if first else offset_of(slot)
                part = fold8(s, jnp.max) + bias_of(role, slot, offset)
            s_ref[pl.ds(c * CHUNK, CHUNK), :] = s
            top = part if top is None else jnp.maximum(top, part)
        x_ref[...] = top

    def stage_softmax(role, group, h, s_ref, x_ref, p_ref, al_ref, first):
        row = role * HEADS + h
        top = jnp.max(x_ref[...], axis=0, keepdims=True)
        if first:
            m = top
        else:
            old = mrun[row, 0:1]
            m = jnp.maximum(old, top)
            alpha = jnp.exp(old - m)
            al_ref[...] = jnp.broadcast_to(alpha, (8, CHUNK))
        mrun[row] = jnp.broadcast_to(m, (8, CHUNK))
        total = None
        for c in range(GROUP):
            slot = GROUP * group + c
            if first and c == 0:
                shift = m
            else:
                shift = m - bias_of(role, slot, OFFSETS[c] if first else offset_of(slot))
            e = jnp.exp(s_ref[pl.ds(c * CHUNK, CHUNK), :] - shift)
            part = fold8(e, jnp.sum)
            total = part if total is None else total + part
            p_ref[pl.ds(c * CHUNK, CHUNK), :] = e.astype(jnp.bfloat16)
        lrun[row] = total if first else lrun[row] * alpha + total

    def stage_pv(role, group, h, row, p_ref, al_ref, first):
        kv = h // SHARE
        out = None
        for c in range(GROUP):
            slot = GROUP * group + c
            p = p_ref[pl.ds(c * CHUNK, CHUNK), :]
            values = vbuf[role, kv, slot]
            if first and c == 0:
                causal = key_ids <= query_ids
                none = jnp.zeros_like(p)
                part = jnp.dot(v_ref[role, kv], jnp.where(causal, p, none), preferred_element_type=jnp.float32)
                part += jnp.dot(values, jnp.where(causal, none, p), preferred_element_type=jnp.float32)
            else:
                part = jnp.dot(values, p, preferred_element_type=jnp.float32)
            out = part if out is None else out + part
        if first:
            acc[row] = out
        else:
            acc[row] = acc[row] * al_ref[0:1] + out

    HALF = HEADS // 2

    def run(first_step, n_steps, first, receive):
        n_units = n_steps * HEADS

        def place(unit):
            step = first_step + unit // HEADS
            return lax.rem(step, 2), step // 2, lax.rem(unit, HEADS)

        def qk(unit, s_ref, x_ref):
            stage_qk(*place(unit), s_ref, x_ref, first)

        def softmax(unit, *refs):
            stage_softmax(*place(unit), *refs, first)

        def pv(unit, row, *refs):
            role, group, h = place(unit)
            stage_pv(role, group, h, row, *refs, first)

        def row_of(unit):
            role, _, h = place(unit)
            return role * HEADS + h

        qk(0, s_a, x_a)

        def body(i, carry):
            receive(i)
            unit = 2 * i
            before = jnp.maximum(unit - 1, 0)
            after = jnp.minimum(unit + 2, n_units - 1)
            qk(unit + 1, s_b, x_b)
            softmax(unit, s_a, x_a, p_a, al_a)
            pv(before, jnp.where(i == 0, 2 * HEADS, row_of(before)), p_b, al_b)
            qk(after, s_a, x_a)
            softmax(unit + 1, s_b, x_b, p_b, al_b)
            pv(unit, row_of(unit), p_a, al_a)
            return carry

        lax.fori_loop(0, n_units // 2, body, 0)
        pv(n_units - 1, row_of(n_units - 1), p_b, al_b)

    receive_direct(0, 0)
    receive_direct(1, 0)
    receive_forwarded(0, 0)

    def receive_first(i):
        @pl.when(i == HALF - 2)
        def _():
            receive_forwarded(1, 0)

    def receive_rest(i):
        for step in range(2 * STEPS - 3):
            @pl.when(i == HALF * step + HALF - 2)
            def _(step=step):
                group, role = divmod(step + 3, 2)
                if step + 4 < 2 * STEPS:
                    ahead, other = divmod(step + 4, 2)
                    receive_direct(other, ahead)
                receive_forwarded(role, group)

    p_b[...] = jnp.zeros_like(p_b)
    al_b[...] = jnp.zeros_like(al_b)
    acc[2 * HEADS] = jnp.zeros((DIM, CHUNK), jnp.float32)
    run(0, 2, True, receive_first)
    receive_direct(0, 1)
    receive_direct(1, 1)
    receive_forwarded(0, 1)
    run(2, 2 * STEPS - 2, False, receive_rest)

    def finish(j, carry):
        for k in range(2):
            row = 2 * j + k
            total = jnp.sum(lrun[row], axis=0, keepdims=True)
            out = (acc[row] * (1.0 / total)).astype(jnp.bfloat16)
            role, h = row // HEADS, lax.rem(row, HEADS)
            o_ref[pl.ds(pl.multiple_of(role * CHUNK, CHUNK), CHUNK), pl.ds(pl.multiple_of(h * DIM, DIM), DIM)] = out.T
        return carry

    lax.fori_loop(0, HEADS, finish, 0)

    for t in NEAR:
        for role in range(2):
            runs, device, band = direct(role, t)

            def drain(role=role, t=t, device=device, band=band):
                for copy in copies(k_ref.at[role], v_ref.at[role], band, SLOT[2 * t], send_sem.at[role, t - 1], device):
                    copy.wait_send()
            when(runs, drain)
    for role in range(2):
        for e in range(0, REACH + 1, 2):
            def drain(role=role, e=e):
                for copy in forward_copies(role, e):
                    copy.wait_send()
            when(forwards(role, e), drain)


def attend(cp, queries, keys, values):
    f32, bf16 = jnp.float32, jnp.bfloat16
    vmem = pl.BlockSpec(memory_space=pltpu.VMEM)
    return pl.pallas_call(
        functools.partial(attention_kernel, cp),
        name="band_attention",
        out_shape=jax.ShapeDtypeStruct(queries.shape, bf16),
        in_specs=[vmem] * 3,
        out_specs=vmem,
        scratch_shapes=[
            pltpu.VMEM((2, KV_HEADS, REACH, CHUNK, DIM), bf16),
            pltpu.VMEM((2, KV_HEADS, REACH, DIM, CHUNK), bf16),
            pltpu.VMEM((GROUP * CHUNK, CHUNK), f32),
            pltpu.VMEM((GROUP * CHUNK, CHUNK), f32),
            pltpu.VMEM((GROUP * CHUNK, CHUNK), bf16),
            pltpu.VMEM((GROUP * CHUNK, CHUNK), bf16),
            pltpu.VMEM((8, CHUNK), f32),
            pltpu.VMEM((8, CHUNK), f32),
            pltpu.VMEM((8, CHUNK), f32),
            pltpu.VMEM((8, CHUNK), f32),
            pltpu.VMEM((2 * HEADS + 1, DIM, CHUNK), f32),
            pltpu.VMEM((2 * HEADS, 8, CHUNK), f32),
            pltpu.VMEM((2 * HEADS, 8, CHUNK), f32),
            pltpu.SemaphoreType.DMA((2, len(NEAR), 2)),
            pltpu.SemaphoreType.DMA((2, REACH // 2 + 1, 2)),
            pltpu.SemaphoreType.DMA((2, REACH, 2)),
        ],
        compiler_params=pltpu.CompilerParams(collective_id=0, has_side_effects=True, vmem_limit_bytes=60 * 1024 * 1024),
    )(queries, keys, values)


def solution(mesh):
    cp = mesh.shape["cp"]

    def device_step(hidden, w_q, w_k, w_v, w_o):
        me = lax.axis_index("cp")
        model_dim = hidden.shape[1]
        x = hidden.reshape(2, CHUNK, model_dim)
        chunk_ids = jnp.stack([me, 2 * cp - 1 - me])
        positions = chunk_ids[:, None] * CHUNK + jnp.arange(CHUNK)[None, :]
        cos_part, sin_part = rotation(positions)
        k_proj = jnp.einsum("nqd,dhe->nqhe", x, w_k, preferred_element_type=jnp.float32).astype(jnp.bfloat16)
        v_proj = jnp.einsum("nqd,dhe->nheq", x, w_v, preferred_element_type=jnp.float32).astype(jnp.bfloat16)
        keys = jnp.transpose(rotate(k_proj, cos_part, sin_part, 1.0), (0, 2, 1, 3))
        q_proj = jnp.einsum("nqd,dhe->nqhe", x, w_q, preferred_element_type=jnp.float32).astype(jnp.bfloat16)
        queries = rotate(q_proj, cos_part, sin_part, DIM ** -0.5).reshape(2 * CHUNK, HEADS * DIM)
        attended = attend(cp, queries, keys, v_proj)
        out = jnp.dot(attended, w_o.reshape(HEADS * DIM, model_dim), preferred_element_type=jnp.float32)
        return out.astype(jnp.bfloat16)

    return jax.shard_map(device_step, mesh=mesh, in_specs=(P(("dp", "cp"), None), P(), P(), P(), P()), out_specs=P(("dp", "cp"), None), check_vma=False)
```

```python
import functools

import jax
import jax.numpy as jnp
from jax import lax
from jax.experimental import pallas as pl
from jax.experimental.pallas import tpu as pltpu
from jax.sharding import PartitionSpec as P

WINDOW = 4096
ROPE_BASE = 10000.0
CHUNK = 256
REACH = WINDOW // CHUNK
GROUP = 4
STEPS = REACH // GROUP
PAIRS = 1
HEADS = 24
KV_HEADS = 2
SHARE = HEADS // KV_HEADS
DIM = 128
NEG = -1e30
HALF = CHUNK // 2
PIECE = 32
MESH = pl.DeviceIdType.MESH

OFFSETS = (16, 8, 2, 1, 6, 10, 9, 7, 14, 15, 4, 3, 12, 5, 11, 13)
SLOT = {offset: slot for slot, offset in enumerate(OFFSETS)}
ROW = 8
SENDS = 8
HEAD_TILE = 8
K_BLOCK = 768


def rotation(positions):
    inv_freq = 1.0 / (ROPE_BASE ** (jnp.arange(DIM // 2, dtype=jnp.float32) * (2.0 / DIM)))
    angles = positions.astype(jnp.float32)[:, None] * inv_freq
    cos_part, sin_part = jnp.cos(angles), jnp.sin(angles)
    return jnp.concatenate([cos_part, cos_part], axis=1), jnp.concatenate([-sin_part, sin_part], axis=1)


def fold8(values, op):
    return op(values.reshape(values.shape[0] // 8, 8, values.shape[1]), axis=0)


def attention_kernel(cp, x_ref, w_ref, k_ref, v_ref, cos_ref, sin_ref, o_ref, q_ref, w_in, w_a, w_b, kbuf, vbuf, s_a, s_b, p_a, p_b, x_a, x_b, al_a, al_b, acc, mrun, lrun, w_sem, send_sem, fwd_sem, recv_sem):
    me = lax.axis_index("cp")
    even_of = (lax.rem(me, 2) == 0, lax.rem(me, 2) == 1)
    partner = me + 1 - 2 * lax.rem(me, 2)
    x_of = (lax.rem(me // 2, 4), 3 - lax.rem(me // 2, 4))

    model_dim = x_ref.shape[1]
    n_blocks = model_dim // K_BLOCK
    n_tiles = HEADS // HEAD_TILE

    def fetch(tile, block, slot):
        rows = pl.ds(pl.multiple_of(block * K_BLOCK, K_BLOCK), K_BLOCK)
        heads = pl.ds(pl.multiple_of(tile * HEAD_TILE, HEAD_TILE), HEAD_TILE)
        return pltpu.make_async_copy(w_ref.at[rows, heads], w_in.at[slot], w_sem.at[slot])

    for slot in range(n_blocks):
        fetch(0, slot, slot).start()

    def later(role, step):
        if role:
            return me >= step, me - step, 1
        low = me + step < cp
        return None, jnp.where(low, me + step, 2 * cp - 1 - me - step), jnp.where(low, 0, 1)

    def beside(role, right):
        at = x_of[role]
        move = jnp.where(at == 3, -6, 2) if right else jnp.where(at == 0, 6, -2)
        return me - move if role else me + move

    def copies(src, band, slot, sems, device):
        for kind, (ref, dst) in enumerate(zip(src, (kbuf, vbuf))):
            yield pltpu.make_async_remote_copy(
                src_ref=ref, dst_ref=dst.at[band, :, slot], send_sem=sems.at[kind], recv_sem=recv_sem.at[band, slot, kind],
                device_id={"cp": device}, device_id_type=MESH)

    def both(*conds):
        conds = [c for c in conds if c is not None]
        return functools.reduce(jnp.logical_and, conds) if conds else None

    def when(cond, fn):
        if cond is None:
            fn()
        else:
            pl.when(cond)(fn)

    def exists(role, offset):
        return None if role or not offset else me >= offset

    def own(role):
        return k_ref.at[role], v_ref.at[role]

    def held(role, offset):
        return (kbuf.at[role, :, SLOT[offset]], vbuf.at[role, :, SLOT[offset]]) if offset else own(role)

    def row_send(role, index, offset, right, dest, only=None):
        return both(only, exists(role, offset)), held(role, offset), role, dest, send_sem.at[role, index], beside(role, right)

    def plans(role, stage):
        at = x_of[role]
        pick = lambda cond, a, b: jnp.where(cond, SLOT[a], SLOT[b])
        if stage == "start":
            for index, step in ((0, ROW), (1, 2 * ROW)):
                there, device, band = later(role, step)
                yield there, own(role), band, SLOT[step], send_sem.at[role, index], device
            yield row_send(role, 4, 0, True, SLOT[2], at < 3)
            yield row_send(role, 5, 0, False, SLOT[6], at == 0)
            yield forward(role, 0)
        elif stage == 8:
            yield row_send(role, 2, 8, True, pick(at < 3, 10, 2))
            yield row_send(role, 3, 8, False, pick(at > 0, 6, 14))
        elif stage == 16:
            yield row_send(role, 4, 16, True, SLOT[10], at == 3)
            yield row_send(role, 5, 16, False, SLOT[14], at > 0)
        elif stage == 2:
            yield row_send(role, 6, 2, True, SLOT[4], at == 2)
        elif stage == 10:
            yield row_send(role, 6, 10, True, pick(at < 2, 12, 4), at != 2)
        elif stage == 6:
            yield row_send(role, 7, 6, False, pick(at == 0, 12, 4), at != 1)
        elif stage == 14:
            yield row_send(role, 7, 14, False, SLOT[12], at == 1)
        if stage != "start":
            yield forward(role, stage)

    def forward(role, e):
        even = even_of[role]
        slot = jnp.where(even, SLOT[min(e + 1, REACH - 1)], SLOT[max(e - 1, 1)])
        only = even if e == 0 else (jnp.logical_not(even) if e == REACH else None)
        return both(only, exists(role, e)), held(role, e), role, slot, fwd_sem.at[role, e // 2], partner

    def launch(role, stage):
        for cond, src, band, slot, sems, device in plans(role, stage):
            def go(src=src, band=band, slot=slot, sems=sems, device=device):
                for copy in copies(src, band, slot, sems, device):
                    copy.start()
            when(cond, go)

    def settle(role, stage):
        for cond, src, band, slot, sems, device in plans(role, stage):
            def go(src=src, band=band, slot=slot, sems=sems, device=device):
                for copy in copies(src, band, slot, sems, device):
                    copy.wait_send()
            when(cond, go)

    def arrive(role, offset):
        def wait():
            for copy in copies(own(role), role, SLOT[offset], send_sem.at[role, 0], partner):
                copy.wait_recv()
        when(exists(role, offset), wait)

    def relay(*offsets):
        for offset in offsets:
            for role in range(2):
                arrive(role, offset)
                launch(role, offset)

    def receive_forwarded(role, group):
        for slot in range(GROUP * group, GROUP * group + GROUP):
            if OFFSETS[slot] % 2:
                arrive(role, OFFSETS[slot])

    for slot, offset in enumerate(OFFSETS):
        @pl.when(me < offset)
        def _(slot=slot):
            kbuf[0, :, slot] = jnp.zeros((KV_HEADS, CHUNK, DIM), jnp.bfloat16)
            vbuf[0, :, slot] = jnp.zeros((KV_HEADS, 2, DIM, HALF), jnp.bfloat16)

    barrier = pltpu.get_barrier_semaphore()

    def greet(device):
        pl.semaphore_signal(barrier, inc=1, device_id={"cp": device}, device_id_type=MESH)

    greet(partner)
    greet(beside(0, True))
    greet(beside(0, False))
    for role in range(2):
        for step in (ROW, 2 * ROW):
            there, device, _ = later(role, step)
            when(there, lambda device=device: greet(device))
    pl.semaphore_wait(barrier, 5 + jnp.where(me >= ROW, 1, 0) + jnp.where(me >= 2 * ROW, 1, 0))
    for role in range(2):
        launch(role, "start")

    def relayout(tile, block, w_out):
        fetch(tile, block, block).wait()
        rows = pl.ds(pl.multiple_of(block * K_BLOCK, K_BLOCK), K_BLOCK)
        w_out[rows, :] = w_in[block].reshape(K_BLOCK, HEAD_TILE * DIM)

    def project(tile, pair, w_two):
        cols = pl.ds(pl.multiple_of(pair * 2 * DIM, 2 * DIM), 2 * DIM)
        found = jnp.dot(x_ref[...], w_two[:, cols], preferred_element_type=jnp.float32).astype(jnp.bfloat16).astype(jnp.float32)
        for k in range(2):
            q = found[:, k * DIM : k * DIM + DIM]
            q = (q * cos_ref[...] + pltpu.roll(q, DIM // 2, 1) * sin_ref[...]) * jnp.float32(DIM ** -0.5)
            q = q.astype(jnp.bfloat16)
            h = tile * HEAD_TILE + 2 * pair + k
            q_ref[h] = q[:CHUNK]
            q_ref[HEADS + h] = q[CHUNK:]

    w_two = (w_a, w_b)
    for tile in range(n_tiles + 1):
        def body(block, carry, tile=tile):
            if tile < n_tiles:
                relayout(tile, block, w_two[tile % 2])
                if tile + 1 < n_tiles:
                    fetch(tile + 1, block, block).start()
            if tile:
                project(tile - 1, block, w_two[(tile - 1) % 2])
            return carry
        lax.fori_loop(0, n_blocks, body, 0)
        if tile == 1:
            relay(8)
    relay(16, 2, 6)

    key_ids = lax.broadcasted_iota(jnp.int32, (CHUNK, CHUNK), 0)
    query_ids = lax.broadcasted_iota(jnp.int32, (CHUNK, CHUNK), 1)

    def query(role, h):
        return q_ref[role * HEADS + h]

    def scores(keys, qh):
        return lax.dot_general(keys, qh, (((1,), (1,)), ((), ())), preferred_element_type=jnp.float32)

    def bias_of(role, slot, offset):
        return jnp.where(jnp.logical_and(role == 0, me < offset), jnp.float32(NEG), jnp.float32(0))

    def offset_of(group, c):
        return jnp.where(group == 1, OFFSETS[GROUP + c], jnp.where(group == 2, OFFSETS[2 * GROUP + c], OFFSETS[3 * GROUP + c]))

    def stage_qk(role, group, h, s_ref, x_ref, first):
        kv = h // SHARE
        qh = query(role, h)
        top = None
        for c in range(GROUP):
            slot = GROUP * group + c
            s = scores(kbuf[role, kv, slot], qh)
            if first and c == 0:
                own = scores(k_ref[role, kv], qh)
                s = jnp.where(key_ids <= query_ids, own, s + bias_of(role, slot, REACH))
                part = fold8(s, jnp.max)
            else:
                offset = OFFSETS[c] if first else offset_of(group, c)
                part = fold8(s, jnp.max) + bias_of(role, slot, offset)
            s_ref[pl.ds(c * CHUNK, CHUNK), :] = s
            top = part if top is None else jnp.maximum(top, part)
        x_ref[...] = top

    def stage_softmax(role, group, h, s_ref, x_ref, p_ref, al_ref, first):
        row = role * HEADS + h
        top = jnp.max(x_ref[...], axis=0, keepdims=True)
        if first:
            m = top
        else:
            old = mrun[row, 0:1]
            m = jnp.maximum(old, top)
            alpha = jnp.exp(old - m)
            al_ref[...] = jnp.broadcast_to(alpha, (8, CHUNK))
        mrun[row] = jnp.broadcast_to(m, (8, CHUNK))
        sums = [None, None]
        for c in range(GROUP):
            slot = GROUP * group + c
            shift = m
            if not (first and c == 0):
                shift = m - bias_of(role, slot, OFFSETS[c] if first else offset_of(group, c))
            for half in range(2):
                cols = slice(half * HALF, half * HALF + HALF)
                for r in range(c * CHUNK, c * CHUNK + CHUNK, PIECE):
                    e = jnp.exp(s_ref[r : r + PIECE, cols] - shift[:, cols])
                    part = fold8(e, jnp.sum)
                    sums[half] = part if sums[half] is None else sums[half] + part
                    p_ref[half, r : r + PIECE] = e.astype(jnp.bfloat16)
        total = jnp.concatenate(sums, axis=1)
        lrun[row] = total if first else lrun[row] * alpha + total

    def stage_pv(role, group, h, row, p_ref, al_ref, first):
        kv = h // SHARE
        out = None
        for c in range(GROUP):
            slot = GROUP * group + c
            rows = slice(c * CHUNK, c * CHUNK + CHUNK)
            p = jnp.concatenate([p_ref[0, rows], p_ref[1, rows]], axis=1)
            values = jnp.concatenate([vbuf[role, kv, slot, 0], vbuf[role, kv, slot, 1]], axis=1)
            if first and c == 0:
                causal = key_ids <= query_ids
                none = jnp.zeros_like(p)
                own = jnp.concatenate([v_ref[role, kv, 0], v_ref[role, kv, 1]], axis=1)
                part = jnp.dot(own, jnp.where(causal, p, none), preferred_element_type=jnp.float32)
                part += jnp.dot(values, jnp.where(causal, none, p), preferred_element_type=jnp.float32)
            else:
                part = jnp.dot(values, p, preferred_element_type=jnp.float32)
            out = part if out is None else out + part
        if first:
            acc[row] = out
        else:
            acc[row] = acc[row] * al_ref[0:1] + out

    TRIPS = HEADS // (2 * PAIRS)

    def run(first_step, n_steps, first, receive):
        n_units = n_steps * HEADS

        def place(unit):
            step = first_step + unit // HEADS
            return lax.rem(step, 2), step // 2, lax.rem(unit, HEADS)

        def qk(unit, s_ref, x_ref):
            stage_qk(*place(unit), s_ref, x_ref, first)

        def softmax(unit, *refs):
            stage_softmax(*place(unit), *refs, first)

        def pv(unit, row, *refs):
            role, group, h = place(unit)
            stage_pv(role, group, h, row, *refs, first)

        def row_of(unit):
            role, _, h = place(unit)
            return role * HEADS + h

        qk(0, s_a, x_a)

        def body(i, carry):
            receive(i)
            for pair in range(PAIRS):
                unit = 2 * (PAIRS * i + pair)
                before = jnp.maximum(unit - 1, 0) if pair == 0 else unit - 1
                after = jnp.minimum(unit + 2, n_units - 1) if pair == PAIRS - 1 else unit + 2
                row = jnp.where(i == 0, 2 * HEADS, row_of(before)) if pair == 0 else row_of(before)
                qk(unit + 1, s_b, x_b)
                softmax(unit, s_a, x_a, p_a, al_a)
                pv(before, row, p_b, al_b)
                qk(after, s_a, x_a)
                softmax(unit + 1, s_b, x_b, p_b, al_b)
                pv(unit, row_of(unit), p_a, al_a)
            return carry

        lax.fori_loop(0, n_units // (2 * PAIRS), body, 0)
        pv(n_units - 1, row_of(n_units - 1), p_b, al_b)

    receive_forwarded(0, 0)

    def at(trip, i, fn):
        @pl.when(i == trip)
        def _():
            fn()

    def receive_first(i):
        at(TRIPS // 2, i, lambda: relay(10))
        at(TRIPS - 1, i, lambda: receive_forwarded(1, 0))
        at(TRIPS + TRIPS // 4, i, lambda: relay(14))

    def receive_rest(i):
        at(0, i, lambda: relay(4))
        at(TRIPS, i, lambda: relay(12))
        for step in range(2 * STEPS - 3):
            group, role = divmod(step + 3, 2)
            at(TRIPS * step + TRIPS - 1, i, lambda role=role, group=group: receive_forwarded(role, group))

    p_b[...] = jnp.zeros_like(p_b)
    al_b[...] = jnp.zeros_like(al_b)
    acc[2 * HEADS] = jnp.zeros((DIM, CHUNK), jnp.float32)
    run(0, 2, True, receive_first)
    receive_forwarded(0, 1)
    run(2, 2 * STEPS - 2, False, receive_rest)

    def finish(j, carry):
        for k in range(2):
            row = 2 * j + k
            total = jnp.sum(lrun[row], axis=0, keepdims=True)
            out = (acc[row] * (1.0 / total)).astype(jnp.bfloat16)
            role, h = row // HEADS, lax.rem(row, HEADS)
            o_ref[pl.ds(pl.multiple_of(role * CHUNK, CHUNK), CHUNK), pl.ds(pl.multiple_of(h * DIM, DIM), DIM)] = out.T
        return carry

    lax.fori_loop(0, HEADS, finish, 0)

    for role in range(2):
        for stage in ("start", 8, 16, 2, 10, 6, 14, 4, 12):
            settle(role, stage)


def project_kernel(x_ref, wk_ref, wv_ref, cos_ref, sin_ref, k_ref, v_ref):
    def product(w_ref):
        w = w_ref[...].reshape(x_ref.shape[1], KV_HEADS * DIM)
        return jnp.dot(x_ref[...], w, preferred_element_type=jnp.float32).astype(jnp.bfloat16)

    k_all = product(wk_ref).astype(jnp.float32)
    v_all = product(wv_ref)
    for kv in range(KV_HEADS):
        k = k_all[:, kv * DIM : kv * DIM + DIM]
        k = (k * cos_ref[...] + pltpu.roll(k, DIM // 2, 1) * sin_ref[...]).astype(jnp.bfloat16)
        v = v_all[:, kv * DIM : kv * DIM + DIM]
        for n in range(2):
            k_ref[n, kv] = k[n * CHUNK : n * CHUNK + CHUNK]
            for half in range(2):
                start = n * CHUNK + half * HALF
                v_ref[n, kv, half] = v[start : start + HALF].T


def project_kv(x, w_k, w_v, cos_part, sin_part):
    return pl.pallas_call(
        project_kernel,
        name="project_kv",
        out_shape=(
            jax.ShapeDtypeStruct((2, KV_HEADS, CHUNK, DIM), jnp.bfloat16),
            jax.ShapeDtypeStruct((2, KV_HEADS, 2, DIM, HALF), jnp.bfloat16),
        ),
        compiler_params=pltpu.CompilerParams(vmem_limit_bytes=48 * 1024 * 1024),
    )(x, w_k, w_v, cos_part, sin_part)


def attend(cp, x, w_q, keys, values, cos_part, sin_part):
    f32, bf16 = jnp.float32, jnp.bfloat16
    vmem = pl.BlockSpec(memory_space=pltpu.VMEM)
    n_blocks = x.shape[1] // K_BLOCK
    return pl.pallas_call(
        functools.partial(attention_kernel, cp),
        name="band_attention",
        out_shape=jax.ShapeDtypeStruct((2 * CHUNK, HEADS * DIM), bf16),
        in_specs=[vmem, pl.BlockSpec(memory_space=pl.ANY), vmem, vmem, vmem, vmem],
        out_specs=vmem,
        scratch_shapes=[
            pltpu.VMEM((2 * HEADS, CHUNK, DIM), bf16),
            pltpu.VMEM((n_blocks, K_BLOCK, HEAD_TILE, DIM), bf16),
            pltpu.VMEM((x.shape[1], HEAD_TILE * DIM), bf16),
            pltpu.VMEM((x.shape[1], HEAD_TILE * DIM), bf16),
            pltpu.VMEM((2, KV_HEADS, REACH, CHUNK, DIM), bf16),
            pltpu.VMEM((2, KV_HEADS, REACH, 2, DIM, HALF), bf16),
            pltpu.VMEM((GROUP * CHUNK, CHUNK), f32),
            pltpu.VMEM((GROUP * CHUNK, CHUNK), f32),
            pltpu.VMEM((2, GROUP * CHUNK, HALF), bf16),
            pltpu.VMEM((2, GROUP * CHUNK, HALF), bf16),
            pltpu.VMEM((8, CHUNK), f32),
            pltpu.VMEM((8, CHUNK), f32),
            pltpu.VMEM((8, CHUNK), f32),
            pltpu.VMEM((8, CHUNK), f32),
            pltpu.VMEM((2 * HEADS + 1, DIM, CHUNK), f32),
            pltpu.VMEM((2 * HEADS, 8, CHUNK), f32),
            pltpu.VMEM((2 * HEADS, 8, CHUNK), f32),
            pltpu.SemaphoreType.DMA((n_blocks,)),
            pltpu.SemaphoreType.DMA((2, SENDS, 2)),
            pltpu.SemaphoreType.DMA((2, REACH // 2 + 1, 2)),
            pltpu.SemaphoreType.DMA((2, REACH, 2)),
        ],
        compiler_params=pltpu.CompilerParams(collective_id=0, has_side_effects=True, vmem_limit_bytes=63 * 1024 * 1024),
    )(x, w_q, keys, values, cos_part, sin_part)


def solution(mesh):
    cp = mesh.shape["cp"]

    def device_step(hidden, w_q, w_k, w_v, w_o):
        me = lax.axis_index("cp")
        chunk_ids = jnp.stack([me, 2 * cp - 1 - me])
        positions = (chunk_ids[:, None] * CHUNK + jnp.arange(CHUNK)[None, :]).reshape(2 * CHUNK)
        cos_part, sin_part = rotation(positions)
        keys, values = project_kv(hidden, w_k, w_v, cos_part, sin_part)
        attended = attend(cp, hidden, w_q, keys, values, cos_part, sin_part)
        out = jnp.dot(attended, w_o.reshape(HEADS * DIM, hidden.shape[1]), preferred_element_type=jnp.float32)
        return out.astype(jnp.bfloat16)

    return jax.shard_map(device_step, mesh=mesh, in_specs=(P(("dp", "cp"), None), P(), P(), P(), P()), out_specs=P(("dp", "cp"), None), check_vma=False)
```

```python
import functools

import jax
import jax.numpy as jnp
from jax import lax
from jax.experimental import pallas as pl
from jax.experimental.pallas import tpu as pltpu
from jax.sharding import PartitionSpec as P

WINDOW = 4096
ROPE_BASE = 10000.0
CHUNK = 256
REACH = WINDOW // CHUNK
GROUP = 4
STEPS = REACH // GROUP
HEADS = 24
KV_HEADS = 2
SHARE = HEADS // KV_HEADS
DIM = 128
NEG = -1e30
HALF = CHUNK // 2
PIECE = 32
MESH = pl.DeviceIdType.MESH

OFFSETS = (16, 8, 2, 1, 6, 10, 9, 7, 14, 15, 4, 3, 12, 5, 11, 13)
SLOT = {offset: slot for slot, offset in enumerate(OFFSETS)}
ROW = 8
SENDS = 8
HEAD_TILE = 8
K_BLOCK = 768
PARTS = 2


def rotation(positions):
    inv_freq = 1.0 / (ROPE_BASE ** (jnp.arange(DIM // 2, dtype=jnp.float32) * (2.0 / DIM)))
    angles = positions.astype(jnp.float32)[:, None] * inv_freq
    cos_part, sin_part = jnp.cos(angles), jnp.sin(angles)
    return jnp.concatenate([cos_part, cos_part], axis=1), jnp.concatenate([-sin_part, sin_part], axis=1)


def fold8(values, op):
    return op(values.reshape(values.shape[0] // 8, 8, values.shape[1]), axis=0)


def attention_kernel(cp, x_ref, w_ref, k_ref, v_ref, cos_ref, sin_ref, o_ref, q_ref, w_in, w_a, w_b, kbuf, vbuf, s_a, s_b, p_a, p_b, f_a, f_b, x_a, x_b, al_a, al_b, acc, mrun, lrun, w_sem, send_sem, fwd_sem, recv_sem):
    me = lax.axis_index("cp")
    even_of = (lax.rem(me, 2) == 0, lax.rem(me, 2) == 1)
    partner = me + 1 - 2 * lax.rem(me, 2)
    x_of = (lax.rem(me // 2, 4), 3 - lax.rem(me // 2, 4))

    model_dim = x_ref.shape[1]
    n_blocks = model_dim // K_BLOCK
    n_tiles = HEADS // HEAD_TILE

    def fetch(tile, block, slot):
        rows = pl.ds(pl.multiple_of(block * K_BLOCK, K_BLOCK), K_BLOCK)
        heads = pl.ds(pl.multiple_of(tile * HEAD_TILE, HEAD_TILE), HEAD_TILE)
        return pltpu.make_async_copy(w_ref.at[rows, heads], w_in.at[slot], w_sem.at[slot])

    for slot in range(n_blocks):
        fetch(0, slot, slot).start()

    def later(role, step):
        if role:
            return me >= step, me - step, 1
        low = me + step < cp
        return None, jnp.where(low, me + step, 2 * cp - 1 - me - step), jnp.where(low, 0, 1)

    def beside(role, right):
        at = x_of[role]
        move = jnp.where(at == 3, -6, 2) if right else jnp.where(at == 0, 6, -2)
        return me - move if role else me + move

    def copies(src, band, slot, sems, device):
        for kind, (ref, dst) in enumerate(zip(src, (kbuf, vbuf))):
            yield pltpu.make_async_remote_copy(
                src_ref=ref, dst_ref=dst.at[band, :, slot], send_sem=sems.at[kind], recv_sem=recv_sem.at[band, slot, kind],
                device_id={"cp": device}, device_id_type=MESH)

    def both(*conds):
        conds = [c for c in conds if c is not None]
        return functools.reduce(jnp.logical_and, conds) if conds else None

    def when(cond, fn):
        if cond is None:
            fn()
        else:
            pl.when(cond)(fn)

    def exists(role, offset):
        return None if role or not offset else me >= offset

    def own(role):
        return k_ref.at[role], v_ref.at[role]

    def held(role, offset):
        return (kbuf.at[role, :, SLOT[offset]], vbuf.at[role, :, SLOT[offset]]) if offset else own(role)

    def row_send(role, index, offset, right, dest, only=None):
        return both(only, exists(role, offset)), held(role, offset), role, dest, send_sem.at[role, index], beside(role, right)

    def plans(role, stage):
        at = x_of[role]
        pick = lambda cond, a, b: jnp.where(cond, SLOT[a], SLOT[b])
        if stage == "start":
            for index, step in ((0, ROW), (1, 2 * ROW)):
                there, device, band = later(role, step)
                yield there, own(role), band, SLOT[step], send_sem.at[role, index], device
            yield row_send(role, 4, 0, True, SLOT[2], at < 3)
            yield row_send(role, 5, 0, False, SLOT[6], at == 0)
            yield forward(role, 0)
        elif stage == 8:
            yield row_send(role, 2, 8, True, pick(at < 3, 10, 2))
            yield row_send(role, 3, 8, False, pick(at > 0, 6, 14))
        elif stage == 16:
            yield row_send(role, 4, 16, True, SLOT[10], at == 3)
            yield row_send(role, 5, 16, False, SLOT[14], at > 0)
        elif stage == 2:
            yield row_send(role, 6, 2, True, SLOT[4], at == 2)
        elif stage == 10:
            yield row_send(role, 6, 10, True, pick(at < 2, 12, 4), at != 2)
        elif stage == 6:
            yield row_send(role, 7, 6, False, pick(at == 0, 12, 4), at != 1)
        elif stage == 14:
            yield row_send(role, 7, 14, False, SLOT[12], at == 1)
        if stage != "start":
            yield forward(role, stage)

    def forward(role, e):
        even = even_of[role]
        slot = jnp.where(even, SLOT[min(e + 1, REACH - 1)], SLOT[max(e - 1, 1)])
        only = even if e == 0 else (jnp.logical_not(even) if e == REACH else None)
        return both(only, exists(role, e)), held(role, e), role, slot, fwd_sem.at[role, e // 2], partner

    def launch(role, stage):
        for cond, src, band, slot, sems, device in plans(role, stage):
            def go(src=src, band=band, slot=slot, sems=sems, device=device):
                for copy in copies(src, band, slot, sems, device):
                    copy.start()
            when(cond, go)

    def settle(role, stage):
        for cond, src, band, slot, sems, device in plans(role, stage):
            def go(src=src, band=band, slot=slot, sems=sems, device=device):
                for copy in copies(src, band, slot, sems, device):
                    copy.wait_send()
            when(cond, go)

    def arrive(role, offset):
        def wait():
            for copy in copies(own(role), role, SLOT[offset], send_sem.at[role, 0], partner):
                copy.wait_recv()
        when(exists(role, offset), wait)

    def relay(*offsets):
        for offset in offsets:
            for role in range(2):
                arrive(role, offset)
                launch(role, offset)

    for slot, offset in enumerate(OFFSETS):
        @pl.when(me < offset)
        def _(slot=slot):
            kbuf[0, :, slot] = jnp.zeros((KV_HEADS, CHUNK, DIM), jnp.bfloat16)
            vbuf[0, :, slot] = jnp.zeros((KV_HEADS, 2, DIM, HALF), jnp.bfloat16)

    barrier = pltpu.get_barrier_semaphore()

    def greet(device):
        pl.semaphore_signal(barrier, inc=1, device_id={"cp": device}, device_id_type=MESH)

    greet(partner)
    greet(beside(0, True))
    greet(beside(0, False))
    for role in range(2):
        for step in (ROW, 2 * ROW):
            there, device, _ = later(role, step)
            when(there, lambda device=device: greet(device))
    pl.semaphore_wait(barrier, 5 + jnp.where(me >= ROW, 1, 0) + jnp.where(me >= 2 * ROW, 1, 0))
    for role in range(2):
        launch(role, "start")

    def relayout(block, part, w_out):
        n = K_BLOCK // PARTS
        rows = pl.ds(pl.multiple_of(block * K_BLOCK + part * n, n), n)
        w_out[rows, :] = w_in[block, part * n : part * n + n].reshape(n, HEAD_TILE * DIM)

    def project(tile, pair, part, w_two):
        cols = pl.ds(pl.multiple_of(pair * 2 * DIM, 2 * DIM), 2 * DIM)
        n = 2 * CHUNK // PARTS
        rows = slice(part * n, part * n + n)
        found = jnp.dot(x_ref[rows, :], w_two[:, cols], preferred_element_type=jnp.float32).astype(jnp.bfloat16).astype(jnp.float32)
        for k in range(2):
            q = found[:, k * DIM : k * DIM + DIM]
            q = (q * cos_ref[rows, :] + pltpu.roll(q, DIM // 2, 1) * sin_ref[rows, :]) * jnp.float32(DIM ** -0.5)
            chunk, start = divmod(part * n, CHUNK)
            q_ref[chunk * HEADS + tile * HEAD_TILE + 2 * pair + k, start : start + n] = q.astype(jnp.bfloat16)

    w_two = (w_a, w_b)
    for tile in range(n_tiles + 1):
        def body(block, carry, tile=tile):
            if tile < n_tiles:
                fetch(tile, block, block).wait()
            for part in range(PARTS):
                if tile:
                    project(tile - 1, block, part, w_two[(tile - 1) % 2])
                if tile < n_tiles:
                    relayout(block, part, w_two[tile % 2])
            if tile + 1 < n_tiles:
                fetch(tile + 1, block, block).start()
            return carry
        lax.fori_loop(0, n_blocks, body, 0)
        if tile == 1:
            relay(8)
    relay(16, 2, 6)

    causal = lax.broadcasted_iota(jnp.int32, (HALF, HALF), 0) <= lax.broadcasted_iota(jnp.int32, (HALF, HALF), 1)
    LOW, HIGH = slice(0, HALF), slice(HALF, CHUNK)

    def scores(keys, qh):
        return lax.dot_general(keys, qh, (((1,), (1,)), ((), ())), preferred_element_type=jnp.float32)

    def bias_of(role, group, c):
        if isinstance(role, int) and role:
            return None
        offset = OFFSETS[GROUP * group + c] if isinstance(group, int) else jnp.where(
            group == 1, OFFSETS[GROUP + c], jnp.where(group == 2, OFFSETS[2 * GROUP + c], OFFSETS[3 * GROUP + c]))
        return jnp.where(jnp.logical_and(role == 0, me < offset), jnp.float32(NEG), jnp.float32(0))

    def plus(value, bias):
        return value if bias is None else value + bias

    def stage_qk(role, group, h, s_ref, x_ref, first):
        kv = h // SHARE
        qh = q_ref[role * HEADS + h]
        top = None
        for c in range(GROUP):
            s = scores(kbuf[role, kv, GROUP * group + c], qh)
            bias = bias_of(role, group, c)
            if first and c == 0:
                own = scores(k_ref[role, kv], qh)
                low = jnp.where(causal, own[LOW, LOW], plus(s[LOW, LOW], bias))
                high = jnp.where(causal, own[HIGH, HIGH], plus(s[HIGH, HIGH], bias))
                s_ref[LOW, LOW] = low
                s_ref[HIGH, HIGH] = high
                s_ref[LOW, HIGH] = own[LOW, HIGH]
                s_ref[HIGH, LOW] = s[HIGH, LOW]
                left = jnp.maximum(fold8(low, jnp.max), plus(fold8(s[HIGH, LOW], jnp.max), bias))
                right = jnp.maximum(fold8(own[LOW, HIGH], jnp.max), fold8(high, jnp.max))
                part = jnp.concatenate([left, right], axis=1)
            else:
                part = plus(fold8(s, jnp.max), bias)
                s_ref[pl.ds(c * CHUNK, CHUNK), :] = s
            top = part if top is None else jnp.maximum(top, part)
            yield
        x_ref[...] = top

    def stage_softmax(role, group, h, s_ref, x_ref, p_ref, al_ref, f_ref, first):
        row = role * HEADS + h
        top = jnp.max(x_ref[...], axis=0, keepdims=True)
        if first:
            m = top
        else:
            old = mrun[row, 0:1]
            m = jnp.maximum(old, top)
            alpha = jnp.exp(old - m)
            al_ref[...] = jnp.broadcast_to(alpha, (8, CHUNK))
        mrun[row] = jnp.broadcast_to(m, (8, CHUNK))
        sums = [None, None]
        for c in range(GROUP):
            bias = bias_of(role, group, c)
            shifted = m if bias is None else m - bias
            for r in range(0, CHUNK, PIECE):
                for half in range(2):
                    cols = slice(half * HALF, half * HALF + HALF)
                    rows = slice(c * CHUNK + r, c * CHUNK + r + PIECE)
                    lower = r >= HALF
                    edge = first and c == 0
                    shift = m if edge and not (lower and half == 0) else shifted
                    e = jnp.exp(s_ref[rows, cols] - shift[:, cols])
                    part = fold8(e, jnp.sum)
                    sums[half] = part if sums[half] is None else sums[half] + part
                    if not edge:
                        p_ref[half, rows] = e.astype(jnp.bfloat16)
                    elif lower and half == 0:
                        f_ref[half, rows] = e.astype(jnp.bfloat16)
                    elif not lower and half == 1:
                        p_ref[half, rows] = e.astype(jnp.bfloat16)
                    else:
                        mask = causal[r % HALF : r % HALF + PIECE]
                        p_ref[half, rows] = jnp.where(mask, e, 0.0).astype(jnp.bfloat16)
                        f_ref[half, rows] = jnp.where(mask, 0.0, e).astype(jnp.bfloat16)
            yield
        total = jnp.concatenate(sums, axis=1)
        lrun[row] = total if first else lrun[row] * alpha + total

    def stage_pv(role, group, h, row, p_ref, al_ref, f_ref, first):
        kv = h // SHARE
        out = None
        for c in range(GROUP):
            slot = GROUP * group + c
            rows = slice(c * CHUNK, c * CHUNK + CHUNK)
            p = jnp.concatenate([p_ref[0, rows], p_ref[1, rows]], axis=1)
            values = jnp.concatenate([vbuf[role, kv, slot, 0], vbuf[role, kv, slot, 1]], axis=1)
            if first and c == 0:
                own = jnp.concatenate([v_ref[role, kv, 0], v_ref[role, kv, 1]], axis=1)
                far = jnp.concatenate([f_ref[0], f_ref[1]], axis=1)
                out = jnp.dot(own, p, preferred_element_type=jnp.float32)
                out += jnp.dot(values, far, preferred_element_type=jnp.float32)
            else:
                part = jnp.dot(values, p, preferred_element_type=jnp.float32)
                out = part if out is None else out + part
            yield
        if first:
            acc[row] = out
        else:
            acc[row] = acc[row] * al_ref[0:1] + out

    TRIPS = HEADS // 2

    def weave(*stages):
        stages = list(stages)
        while stages:
            stages = [stage for stage in stages if next(stage, stages) is None]

    def run(steps, first, ready):
        ready(0)
        weave(stage_qk(*steps[0], 0, s_a, x_a, first))
        for index, (role, group) in enumerate(steps):
            before = steps[index - 1] if index else (role, group)
            after = steps[index + 1] if index + 1 < len(steps) else (role, group)

            def body(i, carry, index=index, role=role, group=group, before=before, after=after):
                if index + 1 < len(steps):
                    @pl.when(i == TRIPS - 1)
                    def _():
                        receive_forwarded(*after)
                h = 2 * i
                head, last = i == 0, i == TRIPS - 1
                pick = lambda cond, a, b: b if isinstance(a, int) and isinstance(b, int) and a == b else jnp.where(cond, a, b)
                b_role, b_group = pick(head, before[0], role), pick(head, before[1], group)
                b_h = jnp.where(head, HEADS - 1, h - 1)
                b_row = b_role * HEADS + b_h
                if index == 0:
                    b_row = jnp.where(head, 2 * HEADS, b_row)
                a_role, a_group = pick(last, after[0], role), pick(last, after[1], group)
                a_h = jnp.where(last, 0, h + 2)
                weave(
                    stage_softmax(role, group, h, s_a, x_a, p_a, al_a, f_a, first),
                    stage_qk(role, group, h + 1, s_b, x_b, first),
                    stage_pv(b_role, b_group, b_h, b_row, p_b, al_b, f_b, first),
                )
                weave(
                    stage_softmax(role, group, h + 1, s_b, x_b, p_b, al_b, f_b, first),
                    stage_qk(a_role, a_group, a_h, s_a, x_a, first),
                    stage_pv(role, group, h, role * HEADS + h, p_a, al_a, f_a, first),
                )
                return carry

            if index:
                ready(index)
            lax.fori_loop(0, TRIPS, body, 0)
        role, group = steps[-1]
        weave(stage_pv(role, group, HEADS - 1, role * HEADS + HEADS - 1, p_b, al_b, f_b, first))

    def receive_forwarded(role, group):
        for offset in OFFSETS[GROUP * group : GROUP * group + GROUP]:
            if offset % 2:
                arrive(role, offset)

    def ready_first(index):
        if index:
            relay(10)

    def ready_rest(index):
        if index == 0:
            relay(14)
            receive_forwarded(0, 1)
        if index == 1:
            relay(4)
        if index == 2:
            relay(12)

    receive_forwarded(0, 0)
    for ref in (p_a, p_b, f_a, f_b, al_b):
        ref[...] = jnp.zeros_like(ref)
    acc[2 * HEADS] = jnp.zeros((DIM, CHUNK), jnp.float32)
    run([(0, 0), (1, 0)], True, ready_first)
    run([(role, group) for group in range(1, STEPS) for role in range(2)], False, ready_rest)

    def finish(j, carry):
        for k in range(2):
            row = 2 * j + k
            total = jnp.sum(lrun[row], axis=0, keepdims=True)
            out = (acc[row] * (1.0 / total)).astype(jnp.bfloat16)
            role, h = row // HEADS, lax.rem(row, HEADS)
            o_ref[pl.ds(pl.multiple_of(role * CHUNK, CHUNK), CHUNK), pl.ds(pl.multiple_of(h * DIM, DIM), DIM)] = out.T
        return carry

    lax.fori_loop(0, HEADS, finish, 0)

    for role in range(2):
        for stage in ("start", 8, 16, 2, 10, 6, 14, 4, 12):
            settle(role, stage)


def project_kernel(x_ref, wk_ref, wv_ref, cos_ref, sin_ref, k_ref, v_ref):
    def product(w_ref):
        w = w_ref[...].reshape(x_ref.shape[1], KV_HEADS * DIM)
        return jnp.dot(x_ref[...], w, preferred_element_type=jnp.float32).astype(jnp.bfloat16)

    k_all = product(wk_ref).astype(jnp.float32)
    v_all = product(wv_ref)
    for kv in range(KV_HEADS):
        k = k_all[:, kv * DIM : kv * DIM + DIM]
        k = (k * cos_ref[...] + pltpu.roll(k, DIM // 2, 1) * sin_ref[...]).astype(jnp.bfloat16)
        v = v_all[:, kv * DIM : kv * DIM + DIM]
        for n in range(2):
            k_ref[n, kv] = k[n * CHUNK : n * CHUNK + CHUNK]
            for half in range(2):
                start = n * CHUNK + half * HALF
                v_ref[n, kv, half] = v[start : start + HALF].T


def project_kv(x, w_k, w_v, cos_part, sin_part):
    return pl.pallas_call(
        project_kernel,
        name="project_kv",
        out_shape=(
            jax.ShapeDtypeStruct((2, KV_HEADS, CHUNK, DIM), jnp.bfloat16),
            jax.ShapeDtypeStruct((2, KV_HEADS, 2, DIM, HALF), jnp.bfloat16),
        ),
        compiler_params=pltpu.CompilerParams(vmem_limit_bytes=48 * 1024 * 1024),
    )(x, w_k, w_v, cos_part, sin_part)


def attend(cp, x, w_q, keys, values, cos_part, sin_part):
    f32, bf16 = jnp.float32, jnp.bfloat16
    vmem = pl.BlockSpec(memory_space=pltpu.VMEM)
    n_blocks = x.shape[1] // K_BLOCK
    return pl.pallas_call(
        functools.partial(attention_kernel, cp),
        name="band_attention",
        out_shape=jax.ShapeDtypeStruct((2 * CHUNK, HEADS * DIM), bf16),
        in_specs=[vmem, pl.BlockSpec(memory_space=pl.ANY), vmem, vmem, vmem, vmem],
        out_specs=vmem,
        scratch_shapes=[
            pltpu.VMEM((2 * HEADS, CHUNK, DIM), bf16),
            pltpu.VMEM((n_blocks, K_BLOCK, HEAD_TILE, DIM), bf16),
            pltpu.VMEM((x.shape[1], HEAD_TILE * DIM), bf16),
            pltpu.VMEM((x.shape[1], HEAD_TILE * DIM), bf16),
            pltpu.VMEM((2, KV_HEADS, REACH, CHUNK, DIM), bf16),
            pltpu.VMEM((2, KV_HEADS, REACH, 2, DIM, HALF), bf16),
            pltpu.VMEM((GROUP * CHUNK, CHUNK), f32),
            pltpu.VMEM((GROUP * CHUNK, CHUNK), f32),
            pltpu.VMEM((2, GROUP * CHUNK, HALF), bf16),
            pltpu.VMEM((2, GROUP * CHUNK, HALF), bf16),
            pltpu.VMEM((2, CHUNK, HALF), bf16),
            pltpu.VMEM((2, CHUNK, HALF), bf16),
            pltpu.VMEM((8, CHUNK), f32),
            pltpu.VMEM((8, CHUNK), f32),
            pltpu.VMEM((8, CHUNK), f32),
            pltpu.VMEM((8, CHUNK), f32),
            pltpu.VMEM((2 * HEADS + 1, DIM, CHUNK), f32),
            pltpu.VMEM((2 * HEADS, 8, CHUNK), f32),
            pltpu.VMEM((2 * HEADS, 8, CHUNK), f32),
            pltpu.SemaphoreType.DMA((n_blocks,)),
            pltpu.SemaphoreType.DMA((2, SENDS, 2)),
            pltpu.SemaphoreType.DMA((2, REACH // 2 + 1, 2)),
            pltpu.SemaphoreType.DMA((2, REACH, 2)),
        ],
        compiler_params=pltpu.CompilerParams(collective_id=0, has_side_effects=True, vmem_limit_bytes=63 * 1024 * 1024),
    )(x, w_q, keys, values, cos_part, sin_part)


def out_kernel(x_ref, w_ref, y_ref):
    y_ref[...] = jnp.dot(x_ref[...], w_ref[...], preferred_element_type=jnp.float32).astype(jnp.bfloat16)


def project_out(attended, w, columns=256):
    rows, depth = attended.shape
    return pl.pallas_call(
        out_kernel,
        name="project_out",
        grid=(w.shape[1] // columns,),
        out_shape=jax.ShapeDtypeStruct((rows, w.shape[1]), jnp.bfloat16),
        in_specs=[pl.BlockSpec((rows, depth), lambda n: (0, 0)), pl.BlockSpec((depth, columns), lambda n: (0, n))],
        out_specs=pl.BlockSpec((rows, columns), lambda n: (0, n)),
        compiler_params=pltpu.CompilerParams(vmem_limit_bytes=48 * 1024 * 1024),
    )(attended, w)


def solution(mesh):
    cp = mesh.shape["cp"]

    def device_step(hidden, w_q, w_k, w_v, w_o):
        me = lax.axis_index("cp")
        chunk_ids = jnp.stack([me, 2 * cp - 1 - me])
        positions = (chunk_ids[:, None] * CHUNK + jnp.arange(CHUNK)[None, :]).reshape(2 * CHUNK)
        cos_part, sin_part = rotation(positions)
        keys, values = project_kv(hidden, w_k, w_v, cos_part, sin_part)
        attended = attend(cp, hidden, w_q, keys, values, cos_part, sin_part)
        return project_out(attended, w_o.reshape(HEADS * DIM, hidden.shape[1]))

    return jax.shard_map(device_step, mesh=mesh, in_specs=(P(("dp", "cp"), None), P(), P(), P(), P()), out_specs=P(("dp", "cp"), None), check_vma=False)
```

```python
import functools

import jax
import jax.numpy as jnp
from jax import lax
from jax.experimental import pallas as pl
from jax.experimental.pallas import tpu as pltpu
from jax.sharding import PartitionSpec as P

WINDOW = 4096
ROPE_BASE = 10000.0
CHUNK = 256
REACH = WINDOW // CHUNK
GROUP = 4
STEPS = REACH // GROUP
HEADS = 24
KV_HEADS = 2
SHARE = HEADS // KV_HEADS
DIM = 128
NEG = -1e30
HALF = CHUNK // 2
PIECE = 32
MESH = pl.DeviceIdType.MESH

OFFSETS = (16, 8, 2, 1, 6, 10, 9, 7, 14, 15, 4, 3, 12, 5, 11, 13)
SLOT = {offset: slot for slot, offset in enumerate(OFFSETS)}
ROW = 8
SENDS = 8
HEAD_TILE = 8
K_BLOCK = 768


def rotation(positions):
    inv_freq = 1.0 / (ROPE_BASE ** (jnp.arange(DIM // 2, dtype=jnp.float32) * (2.0 / DIM)))
    angles = positions.astype(jnp.float32)[:, None] * inv_freq
    cos_part, sin_part = jnp.cos(angles), jnp.sin(angles)
    return jnp.concatenate([cos_part, cos_part], axis=1), jnp.concatenate([-sin_part, sin_part], axis=1)


def fold8(values, op):
    return op(values.reshape(values.shape[0] // 8, 8, values.shape[1]), axis=0)


def attention_kernel(cp, x_ref, w_ref, k_ref, v_ref, cos_ref, sin_ref, o_ref, q_ref, w_in, w_a, w_b, kbuf, vbuf, s_a, s_b, p_a, p_b, f_a, f_b, x_a, x_b, al_a, al_b, acc, mrun, lrun, w_sem, send_sem, fwd_sem, recv_sem):
    me = lax.axis_index("cp")
    even_of = (lax.rem(me, 2) == 0, lax.rem(me, 2) == 1)
    partner = me + 1 - 2 * lax.rem(me, 2)
    x_of = (lax.rem(me // 2, 4), 3 - lax.rem(me // 2, 4))

    model_dim = x_ref.shape[1]
    n_blocks = model_dim // K_BLOCK
    n_tiles = HEADS // HEAD_TILE

    def fetch(tile, block, slot):
        rows = pl.ds(pl.multiple_of(block * K_BLOCK, K_BLOCK), K_BLOCK)
        heads = pl.ds(pl.multiple_of(tile * HEAD_TILE, HEAD_TILE), HEAD_TILE)
        return pltpu.make_async_copy(w_ref.at[rows, heads], w_in.at[slot], w_sem.at[slot])

    for slot in range(n_blocks):
        fetch(0, slot, slot).start()

    def later(role, step):
        if role:
            return me >= step, me - step, 1
        low = me + step < cp
        return None, jnp.where(low, me + step, 2 * cp - 1 - me - step), jnp.where(low, 0, 1)

    def beside(role, right):
        at = x_of[role]
        move = jnp.where(at == 3, -6, 2) if right else jnp.where(at == 0, 6, -2)
        return me - move if role else me + move

    def copies(src, band, slot, sems, device):
        for kind, (ref, dst) in enumerate(zip(src, (kbuf, vbuf))):
            yield pltpu.make_async_remote_copy(
                src_ref=ref, dst_ref=dst.at[band, :, slot], send_sem=sems.at[kind], recv_sem=recv_sem.at[band, slot, kind],
                device_id={"cp": device}, device_id_type=MESH)

    def both(*conds):
        conds = [c for c in conds if c is not None]
        return functools.reduce(jnp.logical_and, conds) if conds else None

    def when(cond, fn):
        if cond is None:
            fn()
        else:
            pl.when(cond)(fn)

    def exists(role, offset):
        return None if role or not offset else me >= offset

    def own(role):
        return k_ref.at[role], v_ref.at[role]

    def held(role, offset):
        return (kbuf.at[role, :, SLOT[offset]], vbuf.at[role, :, SLOT[offset]]) if offset else own(role)

    def row_send(role, index, offset, right, dest, only=None):
        return both(only, exists(role, offset)), held(role, offset), role, dest, send_sem.at[role, index], beside(role, right)

    def plans(role, stage):
        at = x_of[role]
        pick = lambda cond, a, b: jnp.where(cond, SLOT[a], SLOT[b])
        if stage == "start":
            for index, step in ((0, ROW), (1, 2 * ROW)):
                there, device, band = later(role, step)
                yield there, own(role), band, SLOT[step], send_sem.at[role, index], device
            yield row_send(role, 4, 0, True, SLOT[2], at < 3)
            yield row_send(role, 5, 0, False, SLOT[6], at == 0)
            yield forward(role, 0)
        elif stage == 8:
            yield row_send(role, 2, 8, True, pick(at < 3, 10, 2))
            yield row_send(role, 3, 8, False, pick(at > 0, 6, 14))
        elif stage == 16:
            yield row_send(role, 4, 16, True, SLOT[10], at == 3)
            yield row_send(role, 5, 16, False, SLOT[14], at > 0)
        elif stage == 2:
            yield row_send(role, 6, 2, True, SLOT[4], at == 2)
        elif stage == 10:
            yield row_send(role, 6, 10, True, pick(at < 2, 12, 4), at != 2)
        elif stage == 6:
            yield row_send(role, 7, 6, False, pick(at == 0, 12, 4), at != 1)
        elif stage == 14:
            yield row_send(role, 7, 14, False, SLOT[12], at == 1)
        if stage != "start":
            yield forward(role, stage)

    def forward(role, e):
        even = even_of[role]
        slot = jnp.where(even, SLOT[min(e + 1, REACH - 1)], SLOT[max(e - 1, 1)])
        only = even if e == 0 else (jnp.logical_not(even) if e == REACH else None)
        return both(only, exists(role, e)), held(role, e), role, slot, fwd_sem.at[role, e // 2], partner

    def launch(role, stage):
        for cond, src, band, slot, sems, device in plans(role, stage):
            def go(src=src, band=band, slot=slot, sems=sems, device=device):
                for copy in copies(src, band, slot, sems, device):
                    copy.start()
            when(cond, go)

    def settle(role, stage):
        for cond, src, band, slot, sems, device in plans(role, stage):
            def go(src=src, band=band, slot=slot, sems=sems, device=device):
                for copy in copies(src, band, slot, sems, device):
                    copy.wait_send()
            when(cond, go)

    def arrive(role, offset):
        def wait():
            for copy in copies(own(role), role, SLOT[offset], send_sem.at[role, 0], partner):
                copy.wait_recv()
        when(exists(role, offset), wait)

    def relay(*offsets):
        for offset in offsets:
            for role in range(2):
                arrive(role, offset)
                launch(role, offset)

    for slot, offset in enumerate(OFFSETS):
        @pl.when(me < offset)
        def _(slot=slot):
            kbuf[0, :, slot] = jnp.zeros((KV_HEADS, CHUNK, DIM), jnp.bfloat16)
            vbuf[0, :, slot] = jnp.zeros((KV_HEADS, 2, DIM, HALF), jnp.bfloat16)

    barrier = pltpu.get_barrier_semaphore()

    def greet(device):
        pl.semaphore_signal(barrier, inc=1, device_id={"cp": device}, device_id_type=MESH)

    greet(partner)
    greet(beside(0, True))
    greet(beside(0, False))
    for role in range(2):
        for step in (ROW, 2 * ROW):
            there, device, _ = later(role, step)
            when(there, lambda device=device: greet(device))
    pl.semaphore_wait(barrier, 5 + jnp.where(me >= ROW, 1, 0) + jnp.where(me >= 2 * ROW, 1, 0))
    for role in range(2):
        launch(role, "start")

    def relayout(block, w_out):
        rows = pl.ds(pl.multiple_of(block * K_BLOCK, K_BLOCK), K_BLOCK)
        w_out[rows, :] = w_in[block].reshape(K_BLOCK, HEAD_TILE * DIM)

    def project(tile, pair, w_two):
        cols = pl.ds(pl.multiple_of(pair * 2 * DIM, 2 * DIM), 2 * DIM)
        found = jnp.dot(x_ref[...], w_two[:, cols], preferred_element_type=jnp.float32).astype(jnp.bfloat16).astype(jnp.float32)
        for k in range(2):
            q = found[:, k * DIM : k * DIM + DIM]
            q = (q * cos_ref[...] + pltpu.roll(q, DIM // 2, 1) * sin_ref[...]) * jnp.float32(DIM ** -0.5)
            q = q.astype(jnp.bfloat16)
            h = tile * HEAD_TILE + 2 * pair + k
            q_ref[h] = q[:CHUNK]
            q_ref[HEADS + h] = q[CHUNK:]

    w_two = (w_a, w_b)
    for tile in range(n_tiles + 1):
        def body(block, carry, tile=tile):
            if tile < n_tiles:
                fetch(tile, block, block).wait()
            if tile:
                project(tile - 1, block, w_two[(tile - 1) % 2])
            if tile < n_tiles:
                relayout(block, w_two[tile % 2])
            if tile + 1 < n_tiles:
                fetch(tile + 1, block, block).start()
            return carry
        lax.fori_loop(0, n_blocks, body, 0)
        if tile == 1:
            relay(8)
    relay(16, 2, 6)

    causal = lax.broadcasted_iota(jnp.int32, (HALF, HALF), 0) <= lax.broadcasted_iota(jnp.int32, (HALF, HALF), 1)
    LOW, HIGH = slice(0, HALF), slice(HALF, CHUNK)

    def scores(keys, qh):
        return lax.dot_general(keys, qh, (((1,), (1,)), ((), ())), preferred_element_type=jnp.float32)

    def bias_of(role, group, c):
        if isinstance(role, int) and role:
            return None
        offset = OFFSETS[GROUP * group + c] if isinstance(group, int) else jnp.where(
            group == 1, OFFSETS[GROUP + c], jnp.where(group == 2, OFFSETS[2 * GROUP + c], OFFSETS[3 * GROUP + c]))
        return jnp.where(jnp.logical_and(role == 0, me < offset), jnp.float32(NEG), jnp.float32(0))

    def plus(value, bias):
        return value if bias is None else value + bias

    def stage_qk(role, group, h, s_ref, x_ref, first):
        kv = h // SHARE
        qh = q_ref[role * HEADS + h]
        top = None
        for c in range(GROUP):
            s = scores(kbuf[role, kv, GROUP * group + c], qh)
            bias = bias_of(role, group, c)
            if first and c == 0:
                own = scores(k_ref[role, kv], qh)
                low = jnp.where(causal, own[LOW, LOW], plus(s[LOW, LOW], bias))
                high = jnp.where(causal, own[HIGH, HIGH], plus(s[HIGH, HIGH], bias))
                s_ref[LOW, LOW] = low
                s_ref[HIGH, HIGH] = high
                s_ref[LOW, HIGH] = own[LOW, HIGH]
                s_ref[HIGH, LOW] = s[HIGH, LOW]
                left = jnp.maximum(fold8(low, jnp.max), plus(fold8(s[HIGH, LOW], jnp.max), bias))
                right = jnp.maximum(fold8(own[LOW, HIGH], jnp.max), fold8(high, jnp.max))
                part = jnp.concatenate([left, right], axis=1)
            else:
                part = plus(fold8(s, jnp.max), bias)
                s_ref[pl.ds(c * CHUNK, CHUNK), :] = s
            top = part if top is None else jnp.maximum(top, part)
        x_ref[...] = top

    def stage_softmax(role, group, h, s_ref, x_ref, p_ref, al_ref, f_ref, first):
        row = role * HEADS + h
        top = jnp.max(x_ref[...], axis=0, keepdims=True)
        if first:
            m = top
        else:
            old = mrun[row, 0:1]
            m = jnp.maximum(old, top)
            alpha = jnp.exp(old - m)
            al_ref[...] = jnp.broadcast_to(alpha, (8, CHUNK))
        mrun[row] = jnp.broadcast_to(m, (8, CHUNK))
        sums = [None, None]
        for c in range(GROUP):
            bias = bias_of(role, group, c)
            shifted = m if bias is None else m - bias
            for r in range(0, CHUNK, PIECE):
                for half in range(2):
                    cols = slice(half * HALF, half * HALF + HALF)
                    rows = slice(c * CHUNK + r, c * CHUNK + r + PIECE)
                    lower = r >= HALF
                    edge = first and c == 0
                    shift = m if edge and not (lower and half == 0) else shifted
                    e = jnp.exp(s_ref[rows, cols] - shift[:, cols])
                    part = fold8(e, jnp.sum)
                    sums[half] = part if sums[half] is None else sums[half] + part
                    if not edge:
                        p_ref[half, rows] = e.astype(jnp.bfloat16)
                    elif lower and half == 0:
                        f_ref[half, rows] = e.astype(jnp.bfloat16)
                    elif not lower and half == 1:
                        p_ref[half, rows] = e.astype(jnp.bfloat16)
                    else:
                        mask = causal[r % HALF : r % HALF + PIECE]
                        p_ref[half, rows] = jnp.where(mask, e, 0.0).astype(jnp.bfloat16)
                        f_ref[half, rows] = jnp.where(mask, 0.0, e).astype(jnp.bfloat16)
        total = jnp.concatenate(sums, axis=1)
        lrun[row] = total if first else lrun[row] * alpha + total

    def stage_pv(role, group, h, row, p_ref, al_ref, f_ref, first):
        kv = h // SHARE
        out = None
        for c in range(GROUP):
            slot = GROUP * group + c
            rows = slice(c * CHUNK, c * CHUNK + CHUNK)
            p = jnp.concatenate([p_ref[0, rows], p_ref[1, rows]], axis=1)
            values = jnp.concatenate([vbuf[role, kv, slot, 0], vbuf[role, kv, slot, 1]], axis=1)
            if first and c == 0:
                own = jnp.concatenate([v_ref[role, kv, 0], v_ref[role, kv, 1]], axis=1)
                far = jnp.concatenate([f_ref[0], f_ref[1]], axis=1)
                out = jnp.dot(own, p, preferred_element_type=jnp.float32)
                out += jnp.dot(values, far, preferred_element_type=jnp.float32)
            else:
                part = jnp.dot(values, p, preferred_element_type=jnp.float32)
                out = part if out is None else out + part
        if first:
            acc[row] = out
        else:
            acc[row] = acc[row] * al_ref[0:1] + out

    TRIPS = HEADS // 2

    def run(steps, first, ready):
        ready(0)
        stage_qk(*steps[0], 0, s_a, x_a, first)
        for index, (role, group) in enumerate(steps):
            before = steps[index - 1] if index else (role, group)
            after = steps[index + 1] if index + 1 < len(steps) else (role, group)

            def body(i, carry, index=index, role=role, group=group, before=before, after=after):
                if index + 1 < len(steps):
                    @pl.when(i == TRIPS - 1)
                    def _():
                        receive_forwarded(*after)
                h = 2 * i
                head, last = i == 0, i == TRIPS - 1
                pick = lambda cond, a, b: b if isinstance(a, int) and isinstance(b, int) and a == b else jnp.where(cond, a, b)
                b_role, b_group = pick(head, before[0], role), pick(head, before[1], group)
                b_h = jnp.where(head, HEADS - 1, h - 1)
                b_row = b_role * HEADS + b_h
                if index == 0:
                    b_row = jnp.where(head, 2 * HEADS, b_row)
                a_role, a_group = pick(last, after[0], role), pick(last, after[1], group)
                a_h = jnp.where(last, 0, h + 2)
                stage_qk(role, group, h + 1, s_b, x_b, first)
                stage_softmax(role, group, h, s_a, x_a, p_a, al_a, f_a, first)
                stage_pv(b_role, b_group, b_h, b_row, p_b, al_b, f_b, first)
                stage_qk(a_role, a_group, a_h, s_a, x_a, first)
                stage_softmax(role, group, h + 1, s_b, x_b, p_b, al_b, f_b, first)
                stage_pv(role, group, h, role * HEADS + h, p_a, al_a, f_a, first)
                return carry

            if index:
                ready(index)
            lax.fori_loop(0, TRIPS, body, 0)
        role, group = steps[-1]
        stage_pv(role, group, HEADS - 1, role * HEADS + HEADS - 1, p_b, al_b, f_b, first)

    def receive_forwarded(role, group):
        for offset in OFFSETS[GROUP * group : GROUP * group + GROUP]:
            if offset % 2:
                arrive(role, offset)

    def ready_first(index):
        if index:
            relay(10)

    def ready_rest(index):
        if index == 0:
            relay(14)
            receive_forwarded(0, 1)
        if index == 1:
            relay(4)
        if index == 2:
            relay(12)

    receive_forwarded(0, 0)
    for ref in (p_a, p_b, f_a, f_b, al_b):
        ref[...] = jnp.zeros_like(ref)
    acc[2 * HEADS] = jnp.zeros((DIM, CHUNK), jnp.float32)
    run([(0, 0), (1, 0)], True, ready_first)
    run([(role, group) for group in range(1, STEPS) for role in range(2)], False, ready_rest)

    def finish(j, carry):
        for k in range(2):
            row = 2 * j + k
            total = jnp.sum(lrun[row], axis=0, keepdims=True)
            out = (acc[row] * (1.0 / total)).astype(jnp.bfloat16)
            role, h = row // HEADS, lax.rem(row, HEADS)
            o_ref[pl.ds(pl.multiple_of(role * CHUNK, CHUNK), CHUNK), pl.ds(pl.multiple_of(h * DIM, DIM), DIM)] = out.T
        return carry

    lax.fori_loop(0, HEADS, finish, 0)

    for role in range(2):
        for stage in ("start", 8, 16, 2, 10, 6, 14, 4, 12):
            settle(role, stage)


def project_kernel(x_ref, wk_ref, wv_ref, cos_ref, sin_ref, k_ref, v_ref):
    def product(w_ref):
        w = w_ref[...].reshape(x_ref.shape[1], KV_HEADS * DIM)
        return jnp.dot(x_ref[...], w, preferred_element_type=jnp.float32).astype(jnp.bfloat16)

    k_all = product(wk_ref).astype(jnp.float32)
    v_all = product(wv_ref)
    for kv in range(KV_HEADS):
        k = k_all[:, kv * DIM : kv * DIM + DIM]
        k = (k * cos_ref[...] + pltpu.roll(k, DIM // 2, 1) * sin_ref[...]).astype(jnp.bfloat16)
        v = v_all[:, kv * DIM : kv * DIM + DIM]
        for n in range(2):
            k_ref[n, kv] = k[n * CHUNK : n * CHUNK + CHUNK]
            for half in range(2):
                start = n * CHUNK + half * HALF
                v_ref[n, kv, half] = v[start : start + HALF].T


def project_kv(x, w_k, w_v, cos_part, sin_part):
    return pl.pallas_call(
        project_kernel,
        name="project_kv",
        out_shape=(
            jax.ShapeDtypeStruct((2, KV_HEADS, CHUNK, DIM), jnp.bfloat16),
            jax.ShapeDtypeStruct((2, KV_HEADS, 2, DIM, HALF), jnp.bfloat16),
        ),
        compiler_params=pltpu.CompilerParams(vmem_limit_bytes=48 * 1024 * 1024),
    )(x, w_k, w_v, cos_part, sin_part)


def attend(cp, x, w_q, keys, values, cos_part, sin_part):
    f32, bf16 = jnp.float32, jnp.bfloat16
    vmem = pl.BlockSpec(memory_space=pltpu.VMEM)
    n_blocks = x.shape[1] // K_BLOCK
    return pl.pallas_call(
        functools.partial(attention_kernel, cp),
        name="band_attention",
        out_shape=jax.ShapeDtypeStruct((2 * CHUNK, HEADS * DIM), bf16),
        in_specs=[vmem, pl.BlockSpec(memory_space=pl.ANY), vmem, vmem, vmem, vmem],
        out_specs=vmem,
        scratch_shapes=[
            pltpu.VMEM((2 * HEADS, CHUNK, DIM), bf16),
            pltpu.VMEM((n_blocks, K_BLOCK, HEAD_TILE, DIM), bf16),
            pltpu.VMEM((x.shape[1], HEAD_TILE * DIM), bf16),
            pltpu.VMEM((x.shape[1], HEAD_TILE * DIM), bf16),
            pltpu.VMEM((2, KV_HEADS, REACH, CHUNK, DIM), bf16),
            pltpu.VMEM((2, KV_HEADS, REACH, 2, DIM, HALF), bf16),
            pltpu.VMEM((GROUP * CHUNK, CHUNK), f32),
            pltpu.VMEM((GROUP * CHUNK, CHUNK), f32),
            pltpu.VMEM((2, GROUP * CHUNK, HALF), bf16),
            pltpu.VMEM((2, GROUP * CHUNK, HALF), bf16),
            pltpu.VMEM((2, CHUNK, HALF), bf16),
            pltpu.VMEM((2, CHUNK, HALF), bf16),
            pltpu.VMEM((8, CHUNK), f32),
            pltpu.VMEM((8, CHUNK), f32),
            pltpu.VMEM((8, CHUNK), f32),
            pltpu.VMEM((8, CHUNK), f32),
            pltpu.VMEM((2 * HEADS + 1, DIM, CHUNK), f32),
            pltpu.VMEM((2 * HEADS, 8, CHUNK), f32),
            pltpu.VMEM((2 * HEADS, 8, CHUNK), f32),
            pltpu.SemaphoreType.DMA((n_blocks,)),
            pltpu.SemaphoreType.DMA((2, SENDS, 2)),
            pltpu.SemaphoreType.DMA((2, REACH // 2 + 1, 2)),
            pltpu.SemaphoreType.DMA((2, REACH, 2)),
        ],
        compiler_params=pltpu.CompilerParams(collective_id=0, has_side_effects=True, vmem_limit_bytes=63 * 1024 * 1024),
    )(x, w_q, keys, values, cos_part, sin_part)


def solution(mesh):
    cp = mesh.shape["cp"]

    def device_step(hidden, w_q, w_k, w_v, w_o):
        me = lax.axis_index("cp")
        chunk_ids = jnp.stack([me, 2 * cp - 1 - me])
        positions = (chunk_ids[:, None] * CHUNK + jnp.arange(CHUNK)[None, :]).reshape(2 * CHUNK)
        cos_part, sin_part = rotation(positions)
        keys, values = project_kv(hidden, w_k, w_v, cos_part, sin_part)
        attended = attend(cp, hidden, w_q, keys, values, cos_part, sin_part)
        out = jnp.dot(attended, w_o.reshape(HEADS * DIM, hidden.shape[1]), preferred_element_type=jnp.float32)
        return out.astype(jnp.bfloat16)

    return jax.shard_map(device_step, mesh=mesh, in_specs=(P(("dp", "cp"), None), P(), P(), P(), P()), out_specs=P(("dp", "cp"), None), check_vma=False)
```

```python
import functools

import jax
import jax.numpy as jnp
from jax import lax
from jax.experimental import pallas as pl
from jax.experimental.pallas import tpu as pltpu
from jax.sharding import PartitionSpec as P

WINDOW = 4096
ROPE_BASE = 10000.0
CHUNK = 256
REACH = WINDOW // CHUNK
GROUP = 4
STEPS = REACH // GROUP
HEADS = 24
KV_HEADS = 2
PAIRS = 2
SHARE = HEADS // KV_HEADS
DIM = 128
NEG = -1e30
HALF = CHUNK // 2
PIECE = 32
MESH = pl.DeviceIdType.MESH

OFFSETS = (16, 8, 2, 1, 6, 10, 9, 7, 14, 15, 4, 3, 12, 5, 11, 13)
SLOT = {offset: slot for slot, offset in enumerate(OFFSETS)}
ROW = 8
SENDS = 8
HEAD_TILE = 8
K_BLOCK = 768


def rotation(positions):
    inv_freq = 1.0 / (ROPE_BASE ** (jnp.arange(DIM // 2, dtype=jnp.float32) * (2.0 / DIM)))
    angles = positions.astype(jnp.float32)[:, None] * inv_freq
    cos_part, sin_part = jnp.cos(angles), jnp.sin(angles)
    return jnp.concatenate([cos_part, cos_part], axis=1), jnp.concatenate([-sin_part, sin_part], axis=1)


def fold8(values, op):
    return op(values.reshape(values.shape[0] // 8, 8, values.shape[1]), axis=0)


def attention_kernel(cp, x_ref, w_ref, k_ref, v_ref, cos_ref, sin_ref, o_ref, q_ref, w_in, w_a, w_b, kbuf, vbuf, s_a, s_b, p_a, p_b, f_a, f_b, x_a, x_b, al_a, al_b, acc, mrun, lrun, w_sem, send_sem, fwd_sem, recv_sem):
    me = lax.axis_index("cp")
    even_of = (lax.rem(me, 2) == 0, lax.rem(me, 2) == 1)
    partner = me + 1 - 2 * lax.rem(me, 2)
    x_of = (lax.rem(me // 2, 4), 3 - lax.rem(me // 2, 4))

    model_dim = x_ref.shape[1]
    n_blocks = model_dim // K_BLOCK
    n_tiles = HEADS // HEAD_TILE

    def fetch(tile, block, slot):
        rows = pl.ds(pl.multiple_of(block * K_BLOCK, K_BLOCK), K_BLOCK)
        heads = pl.ds(pl.multiple_of(tile * HEAD_TILE, HEAD_TILE), HEAD_TILE)
        return pltpu.make_async_copy(w_ref.at[rows, heads], w_in.at[slot], w_sem.at[slot])

    for slot in range(n_blocks):
        fetch(0, slot, slot).start()

    def later(role, step):
        if role:
            return me >= step, me - step, 1
        low = me + step < cp
        return None, jnp.where(low, me + step, 2 * cp - 1 - me - step), jnp.where(low, 0, 1)

    def beside(role, right):
        at = x_of[role]
        move = jnp.where(at == 3, -6, 2) if right else jnp.where(at == 0, 6, -2)
        return me - move if role else me + move

    def copies(src, band, slot, sems, device):
        for kind, (ref, dst) in enumerate(zip(src, (kbuf, vbuf))):
            yield pltpu.make_async_remote_copy(
                src_ref=ref, dst_ref=dst.at[band, :, slot], send_sem=sems.at[kind], recv_sem=recv_sem.at[band, slot, kind],
                device_id={"cp": device}, device_id_type=MESH)

    def both(*conds):
        conds = [c for c in conds if c is not None]
        return functools.reduce(jnp.logical_and, conds) if conds else None

    def when(cond, fn):
        if cond is None:
            fn()
        else:
            pl.when(cond)(fn)

    def exists(role, offset):
        return None if role or not offset else me >= offset

    def own(role):
        return k_ref.at[role], v_ref.at[role]

    def held(role, offset):
        return (kbuf.at[role, :, SLOT[offset]], vbuf.at[role, :, SLOT[offset]]) if offset else own(role)

    def row_send(role, index, offset, right, dest, only=None):
        return both(only, exists(role, offset)), held(role, offset), role, dest, send_sem.at[role, index], beside(role, right)

    def plans(role, stage):
        at = x_of[role]
        pick = lambda cond, a, b: jnp.where(cond, SLOT[a], SLOT[b])
        if stage == "start":
            for index, step in ((0, ROW), (1, 2 * ROW)):
                there, device, band = later(role, step)
                yield there, own(role), band, SLOT[step], send_sem.at[role, index], device
            yield row_send(role, 4, 0, True, SLOT[2], at < 3)
            yield row_send(role, 5, 0, False, SLOT[6], at == 0)
            yield forward(role, 0)
        elif stage == 8:
            yield row_send(role, 2, 8, True, pick(at < 3, 10, 2))
            yield row_send(role, 3, 8, False, pick(at > 0, 6, 14))
        elif stage == 16:
            yield row_send(role, 4, 16, True, SLOT[10], at == 3)
            yield row_send(role, 5, 16, False, SLOT[14], at > 0)
        elif stage == 2:
            yield row_send(role, 6, 2, True, SLOT[4], at == 2)
        elif stage == 10:
            yield row_send(role, 6, 10, True, pick(at < 2, 12, 4), at != 2)
        elif stage == 6:
            yield row_send(role, 7, 6, False, pick(at == 0, 12, 4), at != 1)
        elif stage == 14:
            yield row_send(role, 7, 14, False, SLOT[12], at == 1)
        if stage != "start":
            yield forward(role, stage)

    def forward(role, e):
        even = even_of[role]
        slot = jnp.where(even, SLOT[min(e + 1, REACH - 1)], SLOT[max(e - 1, 1)])
        only = even if e == 0 else (jnp.logical_not(even) if e == REACH else None)
        return both(only, exists(role, e)), held(role, e), role, slot, fwd_sem.at[role, e // 2], partner

    def launch(role, stage):
        for cond, src, band, slot, sems, device in plans(role, stage):
            def go(src=src, band=band, slot=slot, sems=sems, device=device):
                for copy in copies(src, band, slot, sems, device):
                    copy.start()
            when(cond, go)

    def settle(role, stage):
        for cond, src, band, slot, sems, device in plans(role, stage):
            def go(src=src, band=band, slot=slot, sems=sems, device=device):
                for copy in copies(src, band, slot, sems, device):
                    copy.wait_send()
            when(cond, go)

    def arrive(role, offset):
        def wait():
            for copy in copies(own(role), role, SLOT[offset], send_sem.at[role, 0], partner):
                copy.wait_recv()
        when(exists(role, offset), wait)

    def relay(*offsets):
        for offset in offsets:
            for role in range(2):
                arrive(role, offset)
                launch(role, offset)

    for slot, offset in enumerate(OFFSETS):
        @pl.when(me < offset)
        def _(slot=slot):
            kbuf[0, :, slot] = jnp.zeros((KV_HEADS, CHUNK, DIM), jnp.bfloat16)
            vbuf[0, :, slot] = jnp.zeros((KV_HEADS, 2, DIM, HALF), jnp.bfloat16)

    barrier = pltpu.get_barrier_semaphore()

    def greet(device):
        pl.semaphore_signal(barrier, inc=1, device_id={"cp": device}, device_id_type=MESH)

    greet(partner)
    greet(beside(0, True))
    greet(beside(0, False))
    for role in range(2):
        for step in (ROW, 2 * ROW):
            there, device, _ = later(role, step)
            when(there, lambda device=device: greet(device))
    pl.semaphore_wait(barrier, 5 + jnp.where(me >= ROW, 1, 0) + jnp.where(me >= 2 * ROW, 1, 0))
    for role in range(2):
        launch(role, "start")

    def relayout(block, w_out):
        rows = pl.ds(pl.multiple_of(block * K_BLOCK, K_BLOCK), K_BLOCK)
        w_out[rows, :] = w_in[block].reshape(K_BLOCK, HEAD_TILE * DIM)

    def project(tile, pair, w_two):
        cols = pl.ds(pl.multiple_of(pair * 2 * DIM, 2 * DIM), 2 * DIM)
        found = jnp.dot(x_ref[...], w_two[:, cols], preferred_element_type=jnp.float32).astype(jnp.bfloat16).astype(jnp.float32)
        for k in range(2):
            q = found[:, k * DIM : k * DIM + DIM]
            q = (q * cos_ref[...] + pltpu.roll(q, DIM // 2, 1) * sin_ref[...]) * jnp.float32(DIM ** -0.5)
            q = q.astype(jnp.bfloat16)
            h = tile * HEAD_TILE + 2 * pair + k
            q_ref[h] = q[:CHUNK]
            q_ref[HEADS + h] = q[CHUNK:]

    w_two = (w_a, w_b)
    for tile in range(n_tiles + 1):
        def body(block, carry, tile=tile):
            if tile < n_tiles:
                fetch(tile, block, block).wait()
            if tile:
                project(tile - 1, block, w_two[(tile - 1) % 2])
            if tile < n_tiles:
                relayout(block, w_two[tile % 2])
            if tile + 1 < n_tiles:
                fetch(tile + 1, block, block).start()
            return carry
        lax.fori_loop(0, n_blocks, body, 0)
        if tile == 1:
            relay(8)
    relay(16, 2, 6)

    causal = lax.broadcasted_iota(jnp.int32, (HALF, HALF), 0) <= lax.broadcasted_iota(jnp.int32, (HALF, HALF), 1)
    LOW, HIGH = slice(0, HALF), slice(HALF, CHUNK)

    def scores(keys, qh):
        return lax.dot_general(keys, qh, (((1,), (1,)), ((), ())), preferred_element_type=jnp.float32)

    def bias_of(role, group, c):
        if isinstance(role, int) and role:
            return None
        offset = OFFSETS[GROUP * group + c] if isinstance(group, int) else jnp.where(
            group == 1, OFFSETS[GROUP + c], jnp.where(group == 2, OFFSETS[2 * GROUP + c], OFFSETS[3 * GROUP + c]))
        return jnp.where(jnp.logical_and(role == 0, me < offset), jnp.float32(NEG), jnp.float32(0))

    def plus(value, bias):
        return value if bias is None else value + bias

    def stage_qk(role, group, h, s_ref, x_ref, first):
        kv = h // SHARE
        qh = q_ref[role * HEADS + h]
        top = None
        for c in range(GROUP):
            s = scores(kbuf[role, kv, GROUP * group + c], qh)
            bias = bias_of(role, group, c)
            if first and c == 0:
                own = scores(k_ref[role, kv], qh)
                low = jnp.where(causal, own[LOW, LOW], plus(s[LOW, LOW], bias))
                high = jnp.where(causal, own[HIGH, HIGH], plus(s[HIGH, HIGH], bias))
                s_ref[LOW, LOW] = low
                s_ref[HIGH, HIGH] = high
                s_ref[LOW, HIGH] = own[LOW, HIGH]
                s_ref[HIGH, LOW] = s[HIGH, LOW]
                left = jnp.maximum(fold8(low, jnp.max), plus(fold8(s[HIGH, LOW], jnp.max), bias))
                right = jnp.maximum(fold8(own[LOW, HIGH], jnp.max), fold8(high, jnp.max))
                part = jnp.concatenate([left, right], axis=1)
            else:
                part = plus(fold8(s, jnp.max), bias)
                s_ref[pl.ds(c * CHUNK, CHUNK), :] = s
            top = part if top is None else jnp.maximum(top, part)
        x_ref[...] = top

    def stage_softmax(role, group, h, s_ref, x_ref, p_ref, al_ref, f_ref, first):
        row = role * HEADS + h
        top = jnp.max(x_ref[...], axis=0, keepdims=True)
        if first:
            m = top
        else:
            old = mrun[row, 0:1]
            m = jnp.maximum(old, top)
            alpha = jnp.exp(old - m)
            al_ref[...] = jnp.broadcast_to(alpha, (8, CHUNK))
        mrun[row] = jnp.broadcast_to(m, (8, CHUNK))
        sums = [None, None]
        for c in range(GROUP):
            bias = bias_of(role, group, c)
            shifted = m if bias is None else m - bias
            for r in range(0, CHUNK, PIECE):
                for half in range(2):
                    cols = slice(half * HALF, half * HALF + HALF)
                    rows = slice(c * CHUNK + r, c * CHUNK + r + PIECE)
                    lower = r >= HALF
                    edge = first and c == 0
                    shift = m if edge and not (lower and half == 0) else shifted
                    e = jnp.exp(s_ref[rows, cols] - shift[:, cols])
                    part = fold8(e, jnp.sum)
                    sums[half] = part if sums[half] is None else sums[half] + part
                    if not edge:
                        p_ref[half, rows] = e.astype(jnp.bfloat16)
                    elif lower and half == 0:
                        f_ref[half, rows] = e.astype(jnp.bfloat16)
                    elif not lower and half == 1:
                        p_ref[half, rows] = e.astype(jnp.bfloat16)
                    else:
                        mask = causal[r % HALF : r % HALF + PIECE]
                        p_ref[half, rows] = jnp.where(mask, e, 0.0).astype(jnp.bfloat16)
                        f_ref[half, rows] = jnp.where(mask, 0.0, e).astype(jnp.bfloat16)
        total = jnp.concatenate(sums, axis=1)
        lrun[row] = total if first else lrun[row] * alpha + total

    def stage_pv(role, group, h, row, p_ref, al_ref, f_ref, first):
        kv = h // SHARE
        out = None
        for c in range(GROUP):
            slot = GROUP * group + c
            rows = slice(c * CHUNK, c * CHUNK + CHUNK)
            p = jnp.concatenate([p_ref[0, rows], p_ref[1, rows]], axis=1)
            values = jnp.concatenate([vbuf[role, kv, slot, 0], vbuf[role, kv, slot, 1]], axis=1)
            if first and c == 0:
                own = jnp.concatenate([v_ref[role, kv, 0], v_ref[role, kv, 1]], axis=1)
                far = jnp.concatenate([f_ref[0], f_ref[1]], axis=1)
                out = jnp.dot(own, p, preferred_element_type=jnp.float32)
                out += jnp.dot(values, far, preferred_element_type=jnp.float32)
            else:
                part = jnp.dot(values, p, preferred_element_type=jnp.float32)
                out = part if out is None else out + part
        if first:
            acc[row] = out
        else:
            acc[row] = acc[row] * al_ref[0:1] + out

    TRIPS = HEADS // (2 * PAIRS)

    def step_loop(role, group, before, after, fresh, first, receive):
        def body(i, carry):
            @pl.when(i == TRIPS - 1)
            def _():
                receive()
            head, last = i == 0, i == TRIPS - 1
            pick = lambda cond, a, b: b if isinstance(a, int) and isinstance(b, int) and a == b else jnp.where(cond, a, b)
            for pair in range(PAIRS):
                h = 2 * (PAIRS * i + pair)
                b_role, b_group, b_h, b_row = role, group, h - 1, role * HEADS + h - 1
                a_role, a_group, a_h = role, group, h + 2
                if pair == 0:
                    b_role, b_group = pick(head, before[0], role), pick(head, before[1], group)
                    b_h = jnp.where(head, HEADS - 1, h - 1)
                    b_row = jnp.where(jnp.logical_and(head, fresh), 2 * HEADS, b_role * HEADS + b_h)
                if pair == PAIRS - 1:
                    a_role, a_group = pick(last, after[0], role), pick(last, after[1], group)
                    a_h = jnp.where(last, 0, h + 2)
                stage_qk(role, group, h + 1, s_b, x_b, first)
                stage_softmax(role, group, h, s_a, x_a, p_a, al_a, f_a, first)
                stage_pv(b_role, b_group, b_h, b_row, p_b, al_b, f_b, first)
                stage_qk(a_role, a_group, a_h, s_a, x_a, first)
                stage_softmax(role, group, h + 1, s_b, x_b, p_b, al_b, f_b, first)
                stage_pv(role, group, h, role * HEADS + h, p_a, al_a, f_a, first)
            return carry

        lax.fori_loop(0, TRIPS, body, 0)

    def receive_forwarded(role, group):
        for offset in OFFSETS[GROUP * group : GROUP * group + GROUP]:
            if offset % 2:
                arrive(role, offset)

    receive_forwarded(0, 0)
    for ref in (p_a, p_b, f_a, f_b, al_b):
        ref[...] = jnp.zeros_like(ref)
    acc[2 * HEADS] = jnp.zeros((DIM, CHUNK), jnp.float32)
    stage_qk(0, 0, 0, s_a, x_a, True)
    step_loop(0, 0, (0, 0), (1, 0), True, True, lambda: receive_forwarded(1, 0))
    relay(10)
    step_loop(1, 0, (0, 0), (1, 0), False, True, lambda: None)
    stage_pv(1, 0, HEADS - 1, 2 * HEADS - 1, p_b, al_b, f_b, True)
    relay(14)
    receive_forwarded(0, 1)
    stage_qk(0, 1, 0, s_a, x_a, False)

    def group_loop(group, carry):
        def receive(role, shift):
            for later_group in range(1 + shift, STEPS):
                @pl.when(group + shift == later_group)
                def _(later_group=later_group):
                    receive_forwarded(role, later_group)

        @pl.when(group == 2)
        def _():
            relay(12)
        step_loop(0, group, (1, group - 1), (1, group), group == 1, False, lambda: receive(1, 0))

        @pl.when(group == 1)
        def _():
            relay(4)
        step_loop(1, group, (0, group), (0, jnp.minimum(group + 1, STEPS - 1)), False, False, lambda: receive(0, 1))
        return carry

    lax.fori_loop(1, STEPS, group_loop, 0)
    stage_pv(1, STEPS - 1, HEADS - 1, 2 * HEADS - 1, p_b, al_b, f_b, False)

    def finish(j, carry):
        for k in range(2):
            row = 2 * j + k
            total = jnp.sum(lrun[row], axis=0, keepdims=True)
            out = (acc[row] * (1.0 / total)).astype(jnp.bfloat16)
            role, h = row // HEADS, lax.rem(row, HEADS)
            o_ref[pl.ds(pl.multiple_of(role * CHUNK, CHUNK), CHUNK), pl.ds(pl.multiple_of(h * DIM, DIM), DIM)] = out.T
        return carry

    lax.fori_loop(0, HEADS, finish, 0)

    for role in range(2):
        for stage in ("start", 8, 16, 2, 10, 6, 14, 4, 12):
            settle(role, stage)


def project_kernel(x_ref, wk_ref, wv_ref, cos_ref, sin_ref, k_ref, v_ref):
    def product(w_ref):
        w = w_ref[...].reshape(x_ref.shape[1], KV_HEADS * DIM)
        return jnp.dot(x_ref[...], w, preferred_element_type=jnp.float32).astype(jnp.bfloat16)

    k_all = product(wk_ref).astype(jnp.float32)
    v_all = product(wv_ref)
    for kv in range(KV_HEADS):
        k = k_all[:, kv * DIM : kv * DIM + DIM]
        k = (k * cos_ref[...] + pltpu.roll(k, DIM // 2, 1) * sin_ref[...]).astype(jnp.bfloat16)
        v = v_all[:, kv * DIM : kv * DIM + DIM]
        for n in range(2):
            k_ref[n, kv] = k[n * CHUNK : n * CHUNK + CHUNK]
            for half in range(2):
                start = n * CHUNK + half * HALF
                v_ref[n, kv, half] = v[start : start + HALF].T


def project_kv(x, w_k, w_v, cos_part, sin_part):
    return pl.pallas_call(
        project_kernel,
        name="project_kv",
        out_shape=(
            jax.ShapeDtypeStruct((2, KV_HEADS, CHUNK, DIM), jnp.bfloat16),
            jax.ShapeDtypeStruct((2, KV_HEADS, 2, DIM, HALF), jnp.bfloat16),
        ),
        compiler_params=pltpu.CompilerParams(vmem_limit_bytes=48 * 1024 * 1024),
    )(x, w_k, w_v, cos_part, sin_part)


def attend(cp, x, w_q, keys, values, cos_part, sin_part):
    f32, bf16 = jnp.float32, jnp.bfloat16
    vmem = pl.BlockSpec(memory_space=pltpu.VMEM)
    n_blocks = x.shape[1] // K_BLOCK
    return pl.pallas_call(
        functools.partial(attention_kernel, cp),
        name="band_attention",
        out_shape=jax.ShapeDtypeStruct((2 * CHUNK, HEADS * DIM), bf16),
        in_specs=[vmem, pl.BlockSpec(memory_space=pl.ANY), vmem, vmem, vmem, vmem],
        out_specs=vmem,
        scratch_shapes=[
            pltpu.VMEM((2 * HEADS, CHUNK, DIM), bf16),
            pltpu.VMEM((n_blocks, K_BLOCK, HEAD_TILE, DIM), bf16),
            pltpu.VMEM((x.shape[1], HEAD_TILE * DIM), bf16),
            pltpu.VMEM((x.shape[1], HEAD_TILE * DIM), bf16),
            pltpu.VMEM((2, KV_HEADS, REACH, CHUNK, DIM), bf16),
            pltpu.VMEM((2, KV_HEADS, REACH, 2, DIM, HALF), bf16),
            pltpu.VMEM((GROUP * CHUNK, CHUNK), f32),
            pltpu.VMEM((GROUP * CHUNK, CHUNK), f32),
            pltpu.VMEM((2, GROUP * CHUNK, HALF), bf16),
            pltpu.VMEM((2, GROUP * CHUNK, HALF), bf16),
            pltpu.VMEM((2, CHUNK, HALF), bf16),
            pltpu.VMEM((2, CHUNK, HALF), bf16),
            pltpu.VMEM((8, CHUNK), f32),
            pltpu.VMEM((8, CHUNK), f32),
            pltpu.VMEM((8, CHUNK), f32),
            pltpu.VMEM((8, CHUNK), f32),
            pltpu.VMEM((2 * HEADS + 1, DIM, CHUNK), f32),
            pltpu.VMEM((2 * HEADS, 8, CHUNK), f32),
            pltpu.VMEM((2 * HEADS, 8, CHUNK), f32),
            pltpu.SemaphoreType.DMA((n_blocks,)),
            pltpu.SemaphoreType.DMA((2, SENDS, 2)),
            pltpu.SemaphoreType.DMA((2, REACH // 2 + 1, 2)),
            pltpu.SemaphoreType.DMA((2, REACH, 2)),
        ],
        compiler_params=pltpu.CompilerParams(collective_id=0, has_side_effects=True, vmem_limit_bytes=63 * 1024 * 1024),
    )(x, w_q, keys, values, cos_part, sin_part)


def solution(mesh):
    cp = mesh.shape["cp"]

    def device_step(hidden, w_q, w_k, w_v, w_o):
        me = lax.axis_index("cp")
        chunk_ids = jnp.stack([me, 2 * cp - 1 - me])
        positions = (chunk_ids[:, None] * CHUNK + jnp.arange(CHUNK)[None, :]).reshape(2 * CHUNK)
        cos_part, sin_part = rotation(positions)
        keys, values = project_kv(hidden, w_k, w_v, cos_part, sin_part)
        attended = attend(cp, hidden, w_q, keys, values, cos_part, sin_part)
        out = jnp.dot(attended, w_o.reshape(HEADS * DIM, hidden.shape[1]), preferred_element_type=jnp.float32)
        return out.astype(jnp.bfloat16)

    return jax.shard_map(device_step, mesh=mesh, in_specs=(P(("dp", "cp"), None), P(), P(), P(), P()), out_specs=P(("dp", "cp"), None), check_vma=False)
```

```python
import functools

import jax
import jax.numpy as jnp
from jax import lax
from jax.experimental import pallas as pl
from jax.experimental.pallas import tpu as pltpu
from jax.sharding import PartitionSpec as P

WINDOW = 4096
ROPE_BASE = 10000.0
CHUNK = 256
REACH = WINDOW // CHUNK
GROUP = 4
STEPS = REACH // GROUP
HEADS = 24
KV_HEADS = 2
PAIRS = 3
SHARE = HEADS // KV_HEADS
DIM = 128
NEG = -1e30
HALF = CHUNK // 2
PIECE = 32
MESH = pl.DeviceIdType.MESH

OFFSETS = (16, 8, 2, 1, 6, 10, 9, 7, 14, 15, 4, 3, 12, 5, 11, 13)
SLOT = {offset: slot for slot, offset in enumerate(OFFSETS)}
ROW = 8
SENDS = 8
HEAD_TILE = 8
K_BLOCK = 768


def rotation(positions):
    inv_freq = 1.0 / (ROPE_BASE ** (jnp.arange(DIM // 2, dtype=jnp.float32) * (2.0 / DIM)))
    angles = positions.astype(jnp.float32)[:, None] * inv_freq
    cos_part, sin_part = jnp.cos(angles), jnp.sin(angles)
    return jnp.concatenate([cos_part, cos_part], axis=1), jnp.concatenate([-sin_part, sin_part], axis=1)


def fold8(values, op):
    return op(values.reshape(values.shape[0] // 8, 8, values.shape[1]), axis=0)


def attention_kernel(cp, x_ref, w_ref, k_ref, v_ref, cos_ref, sin_ref, o_ref, q_ref, w_in, w_a, w_b, kbuf, vbuf, s_a, s_b, p_a, p_b, f_a, f_b, x_a, x_b, al_a, al_b, acc, mrun, lrun, w_sem, send_sem, fwd_sem, recv_sem):
    me = lax.axis_index("cp")
    even_of = (lax.rem(me, 2) == 0, lax.rem(me, 2) == 1)
    partner = me + 1 - 2 * lax.rem(me, 2)
    x_of = (lax.rem(me // 2, 4), 3 - lax.rem(me // 2, 4))

    model_dim = x_ref.shape[1]
    n_blocks = model_dim // K_BLOCK
    n_tiles = HEADS // HEAD_TILE

    def fetch(tile, block, slot):
        rows = pl.ds(pl.multiple_of(block * K_BLOCK, K_BLOCK), K_BLOCK)
        heads = pl.ds(pl.multiple_of(tile * HEAD_TILE, HEAD_TILE), HEAD_TILE)
        return pltpu.make_async_copy(w_ref.at[rows, heads], w_in.at[slot], w_sem.at[slot])

    for slot in range(n_blocks):
        fetch(0, slot, slot).start()

    def later(role, step):
        if role:
            return me >= step, me - step, 1
        low = me + step < cp
        return None, jnp.where(low, me + step, 2 * cp - 1 - me - step), jnp.where(low, 0, 1)

    def beside(role, right):
        at = x_of[role]
        move = jnp.where(at == 3, -6, 2) if right else jnp.where(at == 0, 6, -2)
        return me - move if role else me + move

    def copies(src, band, slot, sems, device):
        for kind, (ref, dst) in enumerate(zip(src, (kbuf, vbuf))):
            yield pltpu.make_async_remote_copy(
                src_ref=ref, dst_ref=dst.at[band, :, slot], send_sem=sems.at[kind], recv_sem=recv_sem.at[band, slot, kind],
                device_id={"cp": device}, device_id_type=MESH)

    def both(*conds):
        conds = [c for c in conds if c is not None]
        return functools.reduce(jnp.logical_and, conds) if conds else None

    def when(cond, fn):
        if cond is None:
            fn()
        else:
            pl.when(cond)(fn)

    def exists(role, offset):
        return None if role or not offset else me >= offset

    def own(role):
        return k_ref.at[role], v_ref.at[role]

    def held(role, offset):
        return (kbuf.at[role, :, SLOT[offset]], vbuf.at[role, :, SLOT[offset]]) if offset else own(role)

    def row_send(role, index, offset, right, dest, only=None):
        return both(only, exists(role, offset)), held(role, offset), role, dest, send_sem.at[role, index], beside(role, right)

    def plans(role, stage):
        at = x_of[role]
        pick = lambda cond, a, b: jnp.where(cond, SLOT[a], SLOT[b])
        if stage == "start":
            for index, step in ((0, ROW), (1, 2 * ROW)):
                there, device, band = later(role, step)
                yield there, own(role), band, SLOT[step], send_sem.at[role, index], device
            yield row_send(role, 4, 0, True, SLOT[2], at < 3)
            yield row_send(role, 5, 0, False, SLOT[6], at == 0)
            yield forward(role, 0)
        elif stage == 8:
            yield row_send(role, 2, 8, True, pick(at < 3, 10, 2))
            yield row_send(role, 3, 8, False, pick(at > 0, 6, 14))
        elif stage == 16:
            yield row_send(role, 4, 16, True, SLOT[10], at == 3)
            yield row_send(role, 5, 16, False, SLOT[14], at > 0)
        elif stage == 2:
            yield row_send(role, 6, 2, True, SLOT[4], at == 2)
        elif stage == 10:
            yield row_send(role, 6, 10, True, pick(at < 2, 12, 4), at != 2)
        elif stage == 6:
            yield row_send(role, 7, 6, False, pick(at == 0, 12, 4), at != 1)
        elif stage == 14:
            yield row_send(role, 7, 14, False, SLOT[12], at == 1)
        if stage != "start":
            yield forward(role, stage)

    def forward(role, e):
        even = even_of[role]
        slot = jnp.where(even, SLOT[min(e + 1, REACH - 1)], SLOT[max(e - 1, 1)])
        only = even if e == 0 else (jnp.logical_not(even) if e == REACH else None)
        return both(only, exists(role, e)), held(role, e), role, slot, fwd_sem.at[role, e // 2], partner

    def launch(role, stage):
        for cond, src, band, slot, sems, device in plans(role, stage):
            def go(src=src, band=band, slot=slot, sems=sems, device=device):
                for copy in copies(src, band, slot, sems, device):
                    copy.start()
            when(cond, go)

    def settle(role, stage):
        for cond, src, band, slot, sems, device in plans(role, stage):
            def go(src=src, band=band, slot=slot, sems=sems, device=device):
                for copy in copies(src, band, slot, sems, device):
                    copy.wait_send()
            when(cond, go)

    def arrive(role, offset):
        def wait():
            for copy in copies(own(role), role, SLOT[offset], send_sem.at[role, 0], partner):
                copy.wait_recv()
        when(exists(role, offset), wait)

    def relay(*offsets):
        for offset in offsets:
            for role in range(2):
                arrive(role, offset)
                launch(role, offset)

    for slot, offset in enumerate(OFFSETS):
        @pl.when(me < offset)
        def _(slot=slot):
            kbuf[0, :, slot] = jnp.zeros((KV_HEADS, CHUNK, DIM), jnp.bfloat16)
            vbuf[0, :, slot] = jnp.zeros((KV_HEADS, 2, DIM, HALF), jnp.bfloat16)

    barrier = pltpu.get_barrier_semaphore()

    def greet(device):
        pl.semaphore_signal(barrier, inc=1, device_id={"cp": device}, device_id_type=MESH)

    greet(partner)
    greet(beside(0, True))
    greet(beside(0, False))
    for role in range(2):
        for step in (ROW, 2 * ROW):
            there, device, _ = later(role, step)
            when(there, lambda device=device: greet(device))
    pl.semaphore_wait(barrier, 5 + jnp.where(me >= ROW, 1, 0) + jnp.where(me >= 2 * ROW, 1, 0))
    for role in range(2):
        launch(role, "start")

    def relayout(block, w_out):
        rows = pl.ds(pl.multiple_of(block * K_BLOCK, K_BLOCK), K_BLOCK)
        w_out[rows, :] = w_in[block].reshape(K_BLOCK, HEAD_TILE * DIM)

    def project(tile, pair, w_two):
        cols = pl.ds(pl.multiple_of(pair * 2 * DIM, 2 * DIM), 2 * DIM)
        found = jnp.dot(x_ref[...], w_two[:, cols], preferred_element_type=jnp.float32).astype(jnp.bfloat16).astype(jnp.float32)
        for k in range(2):
            q = found[:, k * DIM : k * DIM + DIM]
            q = (q * cos_ref[...] + pltpu.roll(q, DIM // 2, 1) * sin_ref[...]) * jnp.float32(DIM ** -0.5)
            q = q.astype(jnp.bfloat16)
            h = tile * HEAD_TILE + 2 * pair + k
            q_ref[h] = q[:CHUNK]
            q_ref[HEADS + h] = q[CHUNK:]

    w_two = (w_a, w_b)
    for tile in range(n_tiles + 1):
        def body(block, carry, tile=tile):
            if tile < n_tiles:
                fetch(tile, block, block).wait()
            if tile:
                project(tile - 1, block, w_two[(tile - 1) % 2])
            if tile < n_tiles:
                relayout(block, w_two[tile % 2])
            if tile + 1 < n_tiles:
                fetch(tile + 1, block, block).start()
            return carry
        lax.fori_loop(0, n_blocks, body, 0)
        if tile == 1:
            relay(8)
    relay(16, 2, 6)

    causal = lax.broadcasted_iota(jnp.int32, (HALF, HALF), 0) <= lax.broadcasted_iota(jnp.int32, (HALF, HALF), 1)
    LOW, HIGH = slice(0, HALF), slice(HALF, CHUNK)

    def scores(keys, qh):
        return lax.dot_general(keys, qh, (((1,), (1,)), ((), ())), preferred_element_type=jnp.float32)

    def bias_of(role, group, c):
        if isinstance(role, int) and role:
            return None
        offset = OFFSETS[GROUP * group + c] if isinstance(group, int) else jnp.where(
            group == 1, OFFSETS[GROUP + c], jnp.where(group == 2, OFFSETS[2 * GROUP + c], OFFSETS[3 * GROUP + c]))
        return jnp.where(jnp.logical_and(role == 0, me < offset), jnp.float32(NEG), jnp.float32(0))

    def plus(value, bias):
        return value if bias is None else value + bias

    def stage_qk(role, group, h, s_ref, x_ref, first):
        kv = h // SHARE
        qh = q_ref[role * HEADS + h]
        top = None
        for c in range(GROUP):
            s = scores(kbuf[role, kv, GROUP * group + c], qh)
            bias = bias_of(role, group, c)
            if first and c == 0:
                own = scores(k_ref[role, kv], qh)
                low = jnp.where(causal, own[LOW, LOW], plus(s[LOW, LOW], bias))
                high = jnp.where(causal, own[HIGH, HIGH], plus(s[HIGH, HIGH], bias))
                s_ref[LOW, LOW] = low
                s_ref[HIGH, HIGH] = high
                s_ref[LOW, HIGH] = own[LOW, HIGH]
                s_ref[HIGH, LOW] = s[HIGH, LOW]
                left = jnp.maximum(fold8(low, jnp.max), plus(fold8(s[HIGH, LOW], jnp.max), bias))
                right = jnp.maximum(fold8(own[LOW, HIGH], jnp.max), fold8(high, jnp.max))
                part = jnp.concatenate([left, right], axis=1)
            else:
                part = plus(fold8(s, jnp.max), bias)
                s_ref[pl.ds(c * CHUNK, CHUNK), :] = s
            top = part if top is None else jnp.maximum(top, part)
        x_ref[...] = top

    def stage_softmax(role, group, h, s_ref, x_ref, p_ref, al_ref, f_ref, first):
        row = role * HEADS + h
        top = jnp.max(x_ref[...], axis=0, keepdims=True)
        if first:
            m = top
        else:
            old = mrun[row, 0:1]
            m = jnp.maximum(old, top)
            alpha = jnp.exp(old - m)
            al_ref[...] = jnp.broadcast_to(alpha, (8, CHUNK))
        mrun[row] = jnp.broadcast_to(m, (8, CHUNK))
        sums = [None, None]
        for c in range(GROUP):
            bias = bias_of(role, group, c)
            shifted = m if bias is None else m - bias
            for r in range(0, CHUNK, PIECE):
                for half in range(2):
                    cols = slice(half * HALF, half * HALF + HALF)
                    rows = slice(c * CHUNK + r, c * CHUNK + r + PIECE)
                    lower = r >= HALF
                    edge = first and c == 0
                    shift = m if edge and not (lower and half == 0) else shifted
                    e = jnp.exp(s_ref[rows, cols] - shift[:, cols])
                    part = fold8(e, jnp.sum)
                    sums[half] = part if sums[half] is None else sums[half] + part
                    if not edge:
                        p_ref[half, rows] = e.astype(jnp.bfloat16)
                    elif lower and half == 0:
                        f_ref[half, rows] = e.astype(jnp.bfloat16)
                    elif not lower and half == 1:
                        p_ref[half, rows] = e.astype(jnp.bfloat16)
                    else:
                        mask = causal[r % HALF : r % HALF + PIECE]
                        p_ref[half, rows] = jnp.where(mask, e, 0.0).astype(jnp.bfloat16)
                        f_ref[half, rows] = jnp.where(mask, 0.0, e).astype(jnp.bfloat16)
        total = jnp.concatenate(sums, axis=1)
        lrun[row] = total if first else lrun[row] * alpha + total

    def stage_pv(role, group, h, row, p_ref, al_ref, f_ref, first):
        kv = h // SHARE
        out = None
        for c in range(GROUP):
            slot = GROUP * group + c
            rows = slice(c * CHUNK, c * CHUNK + CHUNK)
            p = jnp.concatenate([p_ref[0, rows], p_ref[1, rows]], axis=1)
            values = jnp.concatenate([vbuf[role, kv, slot, 0], vbuf[role, kv, slot, 1]], axis=1)
            if first and c == 0:
                own = jnp.concatenate([v_ref[role, kv, 0], v_ref[role, kv, 1]], axis=1)
                far = jnp.concatenate([f_ref[0], f_ref[1]], axis=1)
                out = jnp.dot(own, p, preferred_element_type=jnp.float32)
                out += jnp.dot(values, far, preferred_element_type=jnp.float32)
            else:
                part = jnp.dot(values, p, preferred_element_type=jnp.float32)
                out = part if out is None else out + part
        if first:
            acc[row] = out
        else:
            acc[row] = acc[row] * al_ref[0:1] + out

    TRIPS = HEADS // (2 * PAIRS)

    def step_loop(role, group, before, after, fresh, first, receive):
        def body(i, carry):
            @pl.when(i == TRIPS - 1)
            def _():
                receive()
            head, last = i == 0, i == TRIPS - 1
            pick = lambda cond, a, b: b if isinstance(a, int) and isinstance(b, int) and a == b else jnp.where(cond, a, b)
            for pair in range(PAIRS):
                h = 2 * (PAIRS * i + pair)
                b_role, b_group, b_h, b_row = role, group, h - 1, role * HEADS + h - 1
                a_role, a_group, a_h = role, group, h + 2
                if pair == 0:
                    b_role, b_group = pick(head, before[0], role), pick(head, before[1], group)
                    b_h = jnp.where(head, HEADS - 1, h - 1)
                    b_row = jnp.where(jnp.logical_and(head, fresh), 2 * HEADS, b_role * HEADS + b_h)
                if pair == PAIRS - 1:
                    a_role, a_group = pick(last, after[0], role), pick(last, after[1], group)
                    a_h = jnp.where(last, 0, h + 2)
                stage_qk(role, group, h + 1, s_b, x_b, first)
                stage_softmax(role, group, h, s_a, x_a, p_a, al_a, f_a, first)
                stage_pv(b_role, b_group, b_h, b_row, p_b, al_b, f_b, first)
                stage_qk(a_role, a_group, a_h, s_a, x_a, first)
                stage_softmax(role, group, h + 1, s_b, x_b, p_b, al_b, f_b, first)
                stage_pv(role, group, h, role * HEADS + h, p_a, al_a, f_a, first)
            return carry

        lax.fori_loop(0, TRIPS, body, 0)

    def receive_forwarded(role, group):
        for offset in OFFSETS[GROUP * group : GROUP * group + GROUP]:
            if offset % 2:
                arrive(role, offset)

    receive_forwarded(0, 0)
    for ref in (p_a, p_b, f_a, f_b, al_b):
        ref[...] = jnp.zeros_like(ref)
    acc[2 * HEADS] = jnp.zeros((DIM, CHUNK), jnp.float32)
    stage_qk(0, 0, 0, s_a, x_a, True)
    step_loop(0, 0, (0, 0), (1, 0), True, True, lambda: receive_forwarded(1, 0))
    relay(10)
    step_loop(1, 0, (0, 0), (1, 0), False, True, lambda: None)
    stage_pv(1, 0, HEADS - 1, 2 * HEADS - 1, p_b, al_b, f_b, True)
    relay(14)
    receive_forwarded(0, 1)
    stage_qk(0, 1, 0, s_a, x_a, False)

    def group_loop(group, carry):
        def receive(role, shift):
            for later_group in range(1 + shift, STEPS):
                @pl.when(group + shift == later_group)
                def _(later_group=later_group):
                    receive_forwarded(role, later_group)

        @pl.when(group == 2)
        def _():
            relay(12)
        step_loop(0, group, (1, group - 1), (1, group), group == 1, False, lambda: receive(1, 0))

        @pl.when(group == 1)
        def _():
            relay(4)
        step_loop(1, group, (0, group), (0, jnp.minimum(group + 1, STEPS - 1)), False, False, lambda: receive(0, 1))
        return carry

    lax.fori_loop(1, STEPS, group_loop, 0)
    stage_pv(1, STEPS - 1, HEADS - 1, 2 * HEADS - 1, p_b, al_b, f_b, False)

    def finish(j, carry):
        for k in range(2):
            row = 2 * j + k
            total = jnp.sum(lrun[row], axis=0, keepdims=True)
            out = (acc[row] * (1.0 / total)).astype(jnp.bfloat16)
            role, h = row // HEADS, lax.rem(row, HEADS)
            o_ref[pl.ds(pl.multiple_of(role * CHUNK, CHUNK), CHUNK), pl.ds(pl.multiple_of(h * DIM, DIM), DIM)] = out.T
        return carry

    lax.fori_loop(0, HEADS, finish, 0)

    for role in range(2):
        for stage in ("start", 8, 16, 2, 10, 6, 14, 4, 12):
            settle(role, stage)


def project_kernel(x_ref, wk_ref, wv_ref, cos_ref, sin_ref, k_ref, v_ref):
    def product(w_ref):
        w = w_ref[...].reshape(x_ref.shape[1], KV_HEADS * DIM)
        return jnp.dot(x_ref[...], w, preferred_element_type=jnp.float32).astype(jnp.bfloat16)

    k_all = product(wk_ref).astype(jnp.float32)
    v_all = product(wv_ref)
    for kv in range(KV_HEADS):
        k = k_all[:, kv * DIM : kv * DIM + DIM]
        k = (k * cos_ref[...] + pltpu.roll(k, DIM // 2, 1) * sin_ref[...]).astype(jnp.bfloat16)
        v = v_all[:, kv * DIM : kv * DIM + DIM]
        for n in range(2):
            k_ref[n, kv] = k[n * CHUNK : n * CHUNK + CHUNK]
            for half in range(2):
                start = n * CHUNK + half * HALF
                v_ref[n, kv, half] = v[start : start + HALF].T


def project_kv(x, w_k, w_v, cos_part, sin_part):
    return pl.pallas_call(
        project_kernel,
        name="project_kv",
        out_shape=(
            jax.ShapeDtypeStruct((2, KV_HEADS, CHUNK, DIM), jnp.bfloat16),
            jax.ShapeDtypeStruct((2, KV_HEADS, 2, DIM, HALF), jnp.bfloat16),
        ),
        compiler_params=pltpu.CompilerParams(vmem_limit_bytes=48 * 1024 * 1024),
    )(x, w_k, w_v, cos_part, sin_part)


def attend(cp, x, w_q, keys, values, cos_part, sin_part):
    f32, bf16 = jnp.float32, jnp.bfloat16
    vmem = pl.BlockSpec(memory_space=pltpu.VMEM)
    n_blocks = x.shape[1] // K_BLOCK
    return pl.pallas_call(
        functools.partial(attention_kernel, cp),
        name="band_attention",
        out_shape=jax.ShapeDtypeStruct((2 * CHUNK, HEADS * DIM), bf16),
        in_specs=[vmem, pl.BlockSpec(memory_space=pl.ANY), vmem, vmem, vmem, vmem],
        out_specs=vmem,
        scratch_shapes=[
            pltpu.VMEM((2 * HEADS, CHUNK, DIM), bf16),
            pltpu.VMEM((n_blocks, K_BLOCK, HEAD_TILE, DIM), bf16),
            pltpu.VMEM((x.shape[1], HEAD_TILE * DIM), bf16),
            pltpu.VMEM((x.shape[1], HEAD_TILE * DIM), bf16),
            pltpu.VMEM((2, KV_HEADS, REACH, CHUNK, DIM), bf16),
            pltpu.VMEM((2, KV_HEADS, REACH, 2, DIM, HALF), bf16),
            pltpu.VMEM((GROUP * CHUNK, CHUNK), f32),
            pltpu.VMEM((GROUP * CHUNK, CHUNK), f32),
            pltpu.VMEM((2, GROUP * CHUNK, HALF), bf16),
            pltpu.VMEM((2, GROUP * CHUNK, HALF), bf16),
            pltpu.VMEM((2, CHUNK, HALF), bf16),
            pltpu.VMEM((2, CHUNK, HALF), bf16),
            pltpu.VMEM((8, CHUNK), f32),
            pltpu.VMEM((8, CHUNK), f32),
            pltpu.VMEM((8, CHUNK), f32),
            pltpu.VMEM((8, CHUNK), f32),
            pltpu.VMEM((2 * HEADS + 1, DIM, CHUNK), f32),
            pltpu.VMEM((2 * HEADS, 8, CHUNK), f32),
            pltpu.VMEM((2 * HEADS, 8, CHUNK), f32),
            pltpu.SemaphoreType.DMA((n_blocks,)),
            pltpu.SemaphoreType.DMA((2, SENDS, 2)),
            pltpu.SemaphoreType.DMA((2, REACH // 2 + 1, 2)),
            pltpu.SemaphoreType.DMA((2, REACH, 2)),
        ],
        compiler_params=pltpu.CompilerParams(collective_id=0, has_side_effects=True, vmem_limit_bytes=63 * 1024 * 1024),
    )(x, w_q, keys, values, cos_part, sin_part)


def solution(mesh):
    cp = mesh.shape["cp"]

    def device_step(hidden, w_q, w_k, w_v, w_o):
        me = lax.axis_index("cp")
        chunk_ids = jnp.stack([me, 2 * cp - 1 - me])
        positions = (chunk_ids[:, None] * CHUNK + jnp.arange(CHUNK)[None, :]).reshape(2 * CHUNK)
        cos_part, sin_part = rotation(positions)
        keys, values = project_kv(hidden, w_k, w_v, cos_part, sin_part)
        attended = attend(cp, hidden, w_q, keys, values, cos_part, sin_part)
        out = jnp.dot(attended, w_o.reshape(HEADS * DIM, hidden.shape[1]), preferred_element_type=jnp.float32)
        return out.astype(jnp.bfloat16)

    return jax.shard_map(device_step, mesh=mesh, in_specs=(P(("dp", "cp"), None), P(), P(), P(), P()), out_specs=P(("dp", "cp"), None), check_vma=False)
```
